32 devices in a mesh: inst: 1 (over z), qy: 4 (over y), qx: 8 (over x, core).
Axes of the slice: x: 4, y: 4, z: 1, core: 2. Of those that a mesh axis runs over, the one named last changes fastest.
The devices are a block of a 4x4x8 slice.
Arguments:
- cost_diag: float32 [262144], P(('inst', 'qx', 'qy'))
- gamma_angles: float32 [4], replicated
- beta_angles: float32 [4], replicated
Outputs:
- output 1: float32 [1], P('inst')
- output 2: float32 [262144], P(('inst', 'qx', 'qy'))
- output 3: float32 [262144], P(('inst', 'qx', 'qy'))
All inputs are finite; a program needn't handle non-finite values.
Results may differ from the reference program's by a relative error of at most 0.001.
Values sent between devices are 32-bit elements.
A program may use at most 768 MiB of HBM per device.

```python
import math
import jax
import jax.numpy as jnp
from jax import lax

NQUBITS = 18
LAYERS = 4
DEGREE = 2

STATE_LEN = 2 ** NQUBITS
NUM_EDGES = DEGREE * NQUBITS // 2
EXTRA_EDGES = NUM_EDGES - NQUBITS


def draw_edges(key):
    key_first, key_ends, key_step = jax.random.split(key, 3)
    first_ends = jnp.arange(NQUBITS, dtype=jnp.int32)
    first_other = (first_ends + 1 + jax.random.randint(key_first, (NQUBITS,), 0, NQUBITS - 1, dtype=jnp.int32)) % NQUBITS
    extra_ends = jax.random.randint(key_ends, (EXTRA_EDGES,), 0, NQUBITS, dtype=jnp.int32)
    extra_other = (extra_ends + 1 + jax.random.randint(key_step, (EXTRA_EDGES,), 0, NQUBITS - 1, dtype=jnp.int32)) % NQUBITS
    return jnp.concatenate([first_ends, extra_ends]), jnp.concatenate([first_other, extra_other])


def cut_values(ends_a, ends_b, weights):
    index_bits = jnp.arange(STATE_LEN, dtype=jnp.int32)

    def add_edge(edge_idx, cut_sum):
        bit_a = jnp.right_shift(index_bits, ends_a[edge_idx]) & 1
        bit_b = jnp.right_shift(index_bits, ends_b[edge_idx]) & 1
        return cut_sum + weights[edge_idx] * (bit_a ^ bit_b).astype(jnp.float32)

    cut_sum = lax.fori_loop(0, NUM_EDGES, add_edge, jnp.zeros((STATE_LEN,), jnp.float32))
    return cut_sum / math.sqrt(NUM_EDGES)


def setup_inputs(seed: int = 0, part: int = 0) -> dict:
    part_key = jax.random.fold_in(jax.random.key(seed), part)
    key_edges, key_weights = jax.random.split(part_key)
    ends_a, ends_b = draw_edges(key_edges)
    weights = jax.random.uniform(key_weights, (NUM_EDGES,), jnp.float32, 0.5, 1.5)
    key_gamma, key_beta = jax.random.split(jax.random.key(seed + 1))
    gamma_angles = jax.random.uniform(key_gamma, (LAYERS,), jnp.float32, 0.3, 1.0)
    beta_angles = jax.random.uniform(key_beta, (LAYERS,), jnp.float32, 0.4, 1.2)
    return {'cost_diag': cut_values(ends_a, ends_b, weights), 'gamma_angles': gamma_angles, 'beta_angles': beta_angles}


def mixer_gate(amp_re, amp_im, qubit_idx, cos_half, sin_half):
    block_shape = (-1, 2, 2 ** qubit_idx)
    re_blocks = amp_re.reshape(block_shape)
    im_blocks = amp_im.reshape(block_shape)
    new_re = cos_half * re_blocks + sin_half * jnp.flip(im_blocks, axis=1)
    new_im = cos_half * im_blocks - sin_half * jnp.flip(re_blocks, axis=1)
    return new_re.reshape(-1), new_im.reshape(-1)


def reference(cost_diag, gamma_angles, beta_angles):
    start_amp = 2.0 ** (-NQUBITS / 2.0)
    amp_re = jnp.full((STATE_LEN,), start_amp, jnp.float32)
    amp_im = jnp.zeros((STATE_LEN,), jnp.float32)

    def layer_step(layer_state, angles):
        amp_re, amp_im = layer_state
        gamma_one, beta_one = angles
        phase_arg = gamma_one * cost_diag
        cos_t = jnp.cos(phase_arg)
        sin_t = jnp.sin(phase_arg)
        amp_re, amp_im = amp_re * cos_t + amp_im * sin_t, amp_im * cos_t - amp_re * sin_t
        cos_half = jnp.cos(0.5 * beta_one)
        sin_half = jnp.sin(0.5 * beta_one)
        for qubit_idx in range(NQUBITS):
            amp_re, amp_im = mixer_gate(amp_re, amp_im, qubit_idx, cos_half, sin_half)
        return (amp_re, amp_im), None

    (amp_re, amp_im), _unused = lax.scan(layer_step, (amp_re, amp_im), (gamma_angles, beta_angles))
    energy = jnp.sum(cost_diag * (amp_re * amp_re + amp_im * amp_im)).reshape(1)
    return energy, amp_re, amp_im
```

```python
import functools
import math
import jax
import jax.numpy as jnp
from jax import lax
from jax.experimental import pallas as pl
from jax.experimental.pallas import tpu as pltpu
from jax.sharding import PartitionSpec as P

LANES = 128
SIN_POLY = (4.442883014678955, -7.308245658874512, 3.606354236602783, -0.8461116552352905, 0.1098245158791542)
COS_POLY = (1.4142135381698608, -6.9788641929626465, 5.73988151550293, -1.888274908065796, 0.33225154876708984, -0.034501612186431885)
F32 = jnp.float32
BF16 = jnp.bfloat16


def flip_bits(value, mask):
    bit = 1
    while bit <= mask:
        if mask & bit:
            value = value + bit * (1 - 2 * ((value // bit) % 2))
        bit *= 2
    return value


def turn_cos_sin(turns):
    rem = turns - jnp.round(turns)
    sq = rem * rem
    s = SIN_POLY[-1]
    for k in SIN_POLY[-2::-1]:
        s = s * sq + k
    s = s * rem
    c = COS_POLY[-1]
    for k in COS_POLY[-2::-1]:
        c = c * sq + k
    return 1.0 - s * s, s * c


def split3(x):
    a = x.astype(BF16)
    r = x - a.astype(F32)
    b = r.astype(BF16)
    c = (r - b.astype(F32)).astype(BF16)
    return a, b, c


def dot6_lhs(lhs_parts, rhs_cat):
    a, b, c = lhs_parts
    return jnp.dot(jnp.concatenate([a, a, b, a, b, c], axis=1), rhs_cat, preferred_element_type=F32)


def exchange_kernel(half, nqy, cost_ref, table_ref, packet, send_sem, recv_sem):
    me_x, me_y = lax.axis_index('qx'), lax.axis_index('qy')
    barrier = pltpu.get_barrier_semaphore()

    def partner(e):
        return {'qx': flip_bits(me_x, e // nqy), 'qy': flip_bits(me_y, e % nqy)}

    for e in range(1, half):
        pl.semaphore_signal(barrier, inc=1, device_id=partner(e), device_id_type=pl.DeviceIdType.MESH)
    rows = cost_ref.shape[0]
    cost = cost_ref[...]
    rev = reverse_rows(cost)
    col = jnp.concatenate([cost, rev], axis=0).T[0:1, :]
    pk = jnp.concatenate([cost[0:1, :], col, jnp.zeros((6, LANES), F32)], axis=0)
    packet[...] = pk
    table_ref[0, :, :] = pk
    pl.semaphore_wait(barrier, half - 1)
    copies = []
    for e in range(1, half):
        copy = pltpu.make_async_remote_copy(
            src_ref=packet.at[0:2], dst_ref=table_ref.at[e, 0:2], send_sem=send_sem.at[e], recv_sem=recv_sem.at[e],
            device_id=partner(e), device_id_type=pl.DeviceIdType.MESH)
        copy.start()
        copies.append(copy)
    for copy in copies:
        copy.wait()


def reverse_rows(x):
    n = x.shape[0]
    i = lax.broadcasted_iota(jnp.int32, (n, n), 0)
    j = lax.broadcasted_iota(jnp.int32, (n, n), 1)
    perm = jnp.where(i + j == n - 1, 1.0, 0.0).astype(F32)
    return jnp.dot(perm, x, precision=lax.Precision.HIGHEST, preferred_element_type=F32)


def product_matrix(diag, off0, off1, scale):
    lane = lax.broadcasted_iota(jnp.int32, (8, LANES), 1)
    sub = lax.broadcasted_iota(jnp.int32, (8, LANES), 0)
    bit = lambda v, b: (v // (1 << b)) % 2
    base = jnp.full((8, LANES), 1.0, F32) * scale
    rows = [[None, None] for _ in range(7)]
    for b in range(7):
        lb = bit(lane, b) == 1
        row0 = jnp.where(lb, off0, diag[0])
        row1 = jnp.where(lb, diag[1], off1)
        rows[b] = [row0, row1]
    for b in range(3):
        base = base * jnp.where(bit(sub, b) == 1, rows[b][1], rows[b][0])
    blocks = [base]
    for b in range(3, 7):
        blocks = [x * rows[b][0] for x in blocks] + [x * rows[b][1] for x in blocks]
    return jnp.concatenate(blocks, axis=0)


def simulate_kernel(layers, total_bits, gamma_ref, beta_ref, cost_ref, table_ref, energy_ref, re_ref, im_ref,
                    cst, sre, sim):
    rows = cost_ref.shape[0]
    cost = cost_ref[...]
    rev = reverse_rows(cost)
    first = jnp.concatenate([table_ref[e, 0:1, :] - cost[0:1, :] for e in range(16)], axis=0)
    own_col = table_ref[0, 1:2, :]
    cols = jnp.concatenate([table_ref[e, 1:2, :] - own_col for e in range(16)], axis=0)
    cols = cols - cols[:, 0:1]
    cols_t = jnp.concatenate([cols, jnp.zeros((LANES - 16, LANES), F32)], axis=0).T
    for t in range(2):
        for u in range(4):
            for e0s in range(2):
                e = t * 8 + u * 2 + (e0s ^ t)
                base = rev if t else cost
                cst[t, u, e0s * rows:(e0s + 1) * rows, :] = base + (first[e:e + 1, :] + cols_t[t * rows:(t + 1) * rows, e:e + 1])

    lane = lax.broadcasted_iota(jnp.int32, (LANES, LANES), 1)
    vrow = lax.broadcasted_iota(jnp.int32, (LANES, LANES), 0)
    ones = jnp.zeros((LANES, LANES), jnp.int32)
    for b in range(7):
        ones = ones + (lane // (1 << b)) % 2 + (vrow // (1 << b)) % 2
    quarter = (ones % 4).astype(F32) * 0.25

    amp = 2.0 ** (-total_bits / 2.0)
    for l in range(layers):
        g = gamma_ref[l] * (1.0 / (2.0 * math.pi))
        half_beta = jnp.full((8, LANES), 0.5, F32) * beta_ref[l]
        c, s = jnp.cos(half_beta), jnp.sin(half_beta)
        rot = product_matrix((c, c), -s, s, c)
        rot_t = product_matrix((c, c), s, -s, c)
        rk = product_matrix((-s, -s), -c, c, -s)
        rk_t = product_matrix((-s, -s), c, -c, -s)
        w = jnp.concatenate([jnp.concatenate([rot, rk], axis=1), jnp.concatenate([rk, rot], axis=1)], axis=0)
        m = jnp.concatenate([jnp.concatenate([rot_t, rk_t], axis=1), jnp.concatenate([rk_t, rot_t], axis=1)], axis=0)
        w1, w2, w3 = split3(w)
        wcat = jnp.concatenate([w1, w1, w2, w1, w2, w3], axis=1)
        m1, m2, m3 = split3(m)
        mcat = jnp.concatenate([m1, m2, m1, m3, m2, m1], axis=0)
        c2, s2, sc = (c * c)[0:1, :], (s * s)[0:1, :], (s * c)[0:1, :]
        ys = []
        for u in range(4):
            parts = []
            for t in range(2):
                turns = cst[t, u] * g
                if l == 0:
                    turns = turns - jnp.round(turns) - quarter
                    co, si = turn_cos_sin(turns)
                    re, im = amp * co, -amp * si
                else:
                    co, si = turn_cos_sin(turns)
                    a, b = sre[t, u], sim[t, u]
                    re, im = a * co + b * si, b * co - a * si
                parts.append(jnp.concatenate([re, im], axis=1))
            x1, x2, x3 = split3(jnp.concatenate(parts, axis=0))
            xcat = jnp.concatenate([x1, x2, x1, x3, x2, x1], axis=0)
            ys.append(jnp.dot(wcat, xcat, preferred_element_type=F32))
        zs = {}
        for u in range(4):
            y0, y1 = ys[u], ys[3 - u]
            lhs = jnp.concatenate([
                jnp.concatenate([y0[:LANES, :LANES], y1[LANES:, :LANES]], axis=1),
                jnp.concatenate([y0[:LANES, LANES:], y1[LANES:, LANES:]], axis=1)], axis=0)
            z = dot6_lhs(split3(lhs), mcat)
            zs[0, u] = (z[:LANES, :LANES], z[LANES:, :LANES])
            zs[1, 3 - u] = (z[:LANES, LANES:], z[LANES:, LANES:])
        for t in range(2):
            zr = [zs[t, u][0] for u in range(4)]
            zi = [zs[t, u][1] for u in range(4)]
            br = [sc * (zi[1] + zi[2]), sc * (zi[0] + zi[3])]
            bi = [sc * (zr[1] + zr[2]), sc * (zr[0] + zr[3])]
            for u in range(4):
                k = 0 if u in (0, 3) else 1
                sre[t, u] = c2 * zr[u] - s2 * zr[3 - u] + br[k]
                sim[t, u] = c2 * zi[u] - s2 * zi[3 - u] - bi[k]

    total = jnp.zeros((LANES, LANES), F32)
    for t in range(2):
        for u in range(4):
            a, b = sre[t, u], sim[t, u]
            total = total + cst[t, u] * (a * a + b * b)
    energy_ref[...] = jnp.full((8, LANES), 2.0 * jnp.sum(total), F32)
    a, b = sre[0, 0, 0:rows, :], sim[0, 0, 0:rows, :]
    k = ones[0:rows, :] % 4
    re_ref[...] = jnp.where(k == 0, a, jnp.where(k == 1, b, jnp.where(k == 2, -a, -b)))
    im_ref[...] = jnp.where(k == 0, b, jnp.where(k == 1, -a, jnp.where(k == 2, -b, a)))


def solution(mesh):
    nqx, nqy = mesh.shape['qx'], mesh.shape['qy']
    half = nqx * nqy // 2
    state_spec = P(('inst', 'qx', 'qy'))
    vmem = pl.BlockSpec(memory_space=pltpu.VMEM)
    smem = pl.BlockSpec(memory_space=pltpu.SMEM)

    def device_body(cost_loc, gamma_angles, beta_angles):
        local = cost_loc.shape[0]
        rows = local // LANES
        total_bits = int(math.log2(local * nqx * nqy))
        layers = gamma_angles.shape[0]
        cost2 = cost_loc.reshape(rows, LANES)
        table = pl.pallas_call(
            functools.partial(exchange_kernel, half, nqy),
            out_shape=jax.ShapeDtypeStruct((half, 8, LANES), F32),
            in_specs=[vmem], out_specs=vmem,
            scratch_shapes=[pltpu.VMEM((8, LANES), F32), pltpu.SemaphoreType.DMA((half,)), pltpu.SemaphoreType.DMA((half,))],
            compiler_params=pltpu.CompilerParams(collective_id=0, has_side_effects=True),
        )(cost2)
        st = jax.ShapeDtypeStruct((rows, LANES), F32)
        energy, re, im = pl.pallas_call(
            functools.partial(simulate_kernel, layers, total_bits),
            out_shape=(jax.ShapeDtypeStruct((8, LANES), F32), st, st),
            in_specs=[smem, smem, vmem, vmem], out_specs=(vmem, vmem, vmem),
            scratch_shapes=[pltpu.VMEM((2, 4, LANES, LANES), F32)] * 3,
        )(gamma_angles, beta_angles, cost2, table)
        return energy[0, 0:1], re.reshape(local), im.reshape(local)

    return jax.shard_map(device_body, mesh=mesh, in_specs=(state_spec, P(), P()), out_specs=(P('inst'), state_spec, state_spec), check_vma=False)
```

```python
import functools
import math
import jax
import jax.numpy as jnp
from jax import lax
from jax.experimental import pallas as pl
from jax.experimental.pallas import tpu as pltpu
from jax.sharding import PartitionSpec as P

LANES = 128
SIN_POLY = (4.442883014678955, -7.308245658874512, 3.606354236602783, -0.8461116552352905, 0.1098245158791542)
COS_POLY = (1.4142135381698608, -6.9788641929626465, 5.73988151550293, -1.888274908065796, 0.33225154876708984, -0.034501612186431885)
F32 = jnp.float32
BF16 = jnp.bfloat16


def flip_bits(value, mask):
    bit = 1
    while bit <= mask:
        if mask & bit:
            value = value + bit * (1 - 2 * ((value // bit) % 2))
        bit *= 2
    return value


def turn_cos_sin(turns):
    rem = turns - jnp.round(turns)
    sq = rem * rem
    s = SIN_POLY[-1]
    for k in SIN_POLY[-2::-1]:
        s = s * sq + k
    s = s * rem
    c = COS_POLY[-1]
    for k in COS_POLY[-2::-1]:
        c = c * sq + k
    return 1.0 - s * s, s * c


def split3(x):
    a = x.astype(BF16)
    r = x - a.astype(F32)
    b = r.astype(BF16)
    c = (r - b.astype(F32)).astype(BF16)
    return a, b, c


def dot6_lhs(lhs_parts, rhs_cat):
    a, b, c = lhs_parts
    return jnp.dot(jnp.concatenate([a, a, b, a, b, c], axis=1), rhs_cat, preferred_element_type=F32)


def reverse_rows(x):
    n = x.shape[0]
    i = lax.broadcasted_iota(jnp.int32, (n, n), 0)
    j = lax.broadcasted_iota(jnp.int32, (n, n), 1)
    perm = jnp.where(i + j == n - 1, 1.0, 0.0).astype(F32)
    return jnp.dot(perm, x, precision=lax.Precision.HIGHEST, preferred_element_type=F32)


def product_matrix(diag, off0, off1, scale):
    lane = lax.broadcasted_iota(jnp.int32, (8, LANES), 1)
    sub = lax.broadcasted_iota(jnp.int32, (8, LANES), 0)
    bit = lambda v, b: (v // (1 << b)) % 2
    base = jnp.full((8, LANES), 1.0, F32) * scale
    rows = [[None, None] for _ in range(7)]
    for b in range(7):
        lb = bit(lane, b) == 1
        row0 = jnp.where(lb, off0, diag[0])
        row1 = jnp.where(lb, diag[1], off1)
        rows[b] = [row0, row1]
    for b in range(3):
        base = base * jnp.where(bit(sub, b) == 1, rows[b][1], rows[b][0])
    blocks = [base]
    for b in range(3, 7):
        blocks = [x * rows[b][0] for x in blocks] + [x * rows[b][1] for x in blocks]
    return jnp.concatenate(blocks, axis=0)


def kernel(layers, total_bits, half, nqy, gamma_ref, beta_ref, cost_hbm, energy_ref, re_ref, im_ref,
           cost_ref, table_ref, packet, cst, sre, sim, wcat_ref, mcat_ref, load_sem, send_sem, recv_sem):
    load = pltpu.make_async_copy(cost_hbm, cost_ref, load_sem)
    load.start()
    me_x, me_y = lax.axis_index('qx'), lax.axis_index('qy')
    barrier = pltpu.get_barrier_semaphore()

    def partner(e):
        return {'qx': flip_bits(me_x, e // nqy), 'qy': flip_bits(me_y, e % nqy)}

    for e in range(1, half):
        pl.semaphore_signal(barrier, inc=1, device_id=partner(e), device_id_type=pl.DeviceIdType.MESH)
    load.wait()
    rows = cost_ref.shape[0]
    cost = cost_ref[...]
    rev = reverse_rows(cost)
    col = jnp.concatenate([cost, rev], axis=0).T[0:1, :]
    packet[0:1, :] = cost[0:1, :]
    packet[1:2, :] = col
    pl.semaphore_wait(barrier, half - 1)
    copies = []
    for e in range(1, half):
        copy = pltpu.make_async_remote_copy(
            src_ref=packet.at[0:2], dst_ref=table_ref.at[e, 0:2], send_sem=send_sem.at[e], recv_sem=recv_sem.at[e],
            device_id=partner(e), device_id_type=pl.DeviceIdType.MESH)
        copy.start()
        copies.append(copy)
    trig = []
    for l in range(layers):
        half_beta = jnp.full((8, LANES), 0.5, F32) * beta_ref[l]
        c, s = jnp.cos(half_beta), jnp.sin(half_beta)
        rot = product_matrix((c, c), -s, s, c)
        rot_t = product_matrix((c, c), s, -s, c)
        rk = product_matrix((-s, -s), -c, c, -s)
        rk_t = product_matrix((-s, -s), c, -c, -s)
        w = jnp.concatenate([jnp.concatenate([rot, rk], axis=1), jnp.concatenate([rk, rot], axis=1)], axis=0)
        m = jnp.concatenate([jnp.concatenate([rot_t, rk_t], axis=1), jnp.concatenate([rk_t, rot_t], axis=1)], axis=0)
        for k, part in enumerate(split3(w)):
            wcat_ref[l, k] = part
        for k, part in enumerate(split3(m)):
            mcat_ref[l, k] = part
        trig.append(((c * c)[0:1, :], (s * s)[0:1, :], (s * c)[0:1, :]))

    lane = lax.broadcasted_iota(jnp.int32, (LANES, LANES), 1)
    vrow = lax.broadcasted_iota(jnp.int32, (LANES, LANES), 0)
    ones = jnp.zeros((LANES, LANES), jnp.int32)
    for b in range(7):
        ones = ones + (lane // (1 << b)) % 2 + (vrow // (1 << b)) % 2
    quarter = (ones % 4).astype(F32) * 0.25

    for copy in copies:
        copy.wait()
    first = jnp.concatenate([(table_ref[e, 0:1, :] - cost[0:1, :]) if e else jnp.zeros((1, LANES), F32) for e in range(16)], axis=0)
    own_col = col
    cols = jnp.concatenate([(table_ref[e, 1:2, :] - own_col) if e else jnp.zeros((1, LANES), F32) for e in range(16)], axis=0)
    cols = cols - cols[:, 0:1]
    cols_t = jnp.concatenate([cols, jnp.zeros((LANES - 16, LANES), F32)], axis=0).T
    for t in range(2):
        for u in range(4):
            for e0s in range(2):
                e = t * 8 + u * 2 + (e0s ^ t)
                base = rev if t else cost
                cst[t, u, e0s * rows:(e0s + 1) * rows, :] = base + (first[e:e + 1, :] + cols_t[t * rows:(t + 1) * rows, e:e + 1])

    amp = 2.0 ** (-total_bits / 2.0)
    for l in range(layers):
        g = gamma_ref[l] * (1.0 / (2.0 * math.pi))
        w1, w2, w3 = [wcat_ref[l, k] for k in range(3)]
        wcat = jnp.concatenate([w1, w1, w2, w1, w2, w3], axis=1)
        m1, m2, m3 = [mcat_ref[l, k] for k in range(3)]
        mcat = jnp.concatenate([m1, m2, m1, m3, m2, m1], axis=0)
        c2, s2, sc = trig[l]
        ys = []
        for u in range(4):
            parts = []
            for t in range(2):
                turns = cst[t, u] * g
                if l == 0:
                    turns = turns - jnp.round(turns) - quarter
                    co, si = turn_cos_sin(turns)
                    re, im = amp * co, -amp * si
                else:
                    co, si = turn_cos_sin(turns)
                    a, b = sre[t, u], sim[t, u]
                    re, im = a * co + b * si, b * co - a * si
                parts.append(jnp.concatenate([re, im], axis=1))
            x1, x2, x3 = split3(jnp.concatenate(parts, axis=0))
            xcat = jnp.concatenate([x1, x2, x1, x3, x2, x1], axis=0)
            ys.append(jnp.dot(wcat, xcat, preferred_element_type=F32))
        zs = {}
        for u in range(4):
            y0, y1 = ys[u], ys[3 - u]
            lhs = jnp.concatenate([
                jnp.concatenate([y0[:LANES, :LANES], y1[LANES:, :LANES]], axis=1),
                jnp.concatenate([y0[:LANES, LANES:], y1[LANES:, LANES:]], axis=1)], axis=0)
            z = dot6_lhs(split3(lhs), mcat)
            zs[0, u] = (z[:LANES, :LANES], z[LANES:, :LANES])
            zs[1, 3 - u] = (z[:LANES, LANES:], z[LANES:, LANES:])
        for t in range(2):
            zr = [zs[t, u][0] for u in range(4)]
            zi = [zs[t, u][1] for u in range(4)]
            br = [sc * (zi[1] + zi[2]), sc * (zi[0] + zi[3])]
            bi = [sc * (zr[1] + zr[2]), sc * (zr[0] + zr[3])]
            for u in range(4):
                k = 0 if u in (0, 3) else 1
                sre[t, u] = c2 * zr[u] - s2 * zr[3 - u] + br[k]
                sim[t, u] = c2 * zi[u] - s2 * zi[3 - u] - bi[k]

    total = jnp.zeros((LANES, LANES), F32)
    for t in range(2):
        for u in range(4):
            a, b = sre[t, u], sim[t, u]
            total = total + cst[t, u] * (a * a + b * b)
    energy_ref[0] = 2.0 * jnp.sum(total)
    a, b = sre[0, 0, 0:rows, :], sim[0, 0, 0:rows, :]
    k = ones[0:rows, :] % 4
    re_ref[...] = jnp.where(k == 0, a, jnp.where(k == 1, b, jnp.where(k == 2, -a, -b)))
    im_ref[...] = jnp.where(k == 0, b, jnp.where(k == 1, -a, jnp.where(k == 2, -b, a)))


def solution(mesh):
    nqx, nqy = mesh.shape['qx'], mesh.shape['qy']
    half = nqx * nqy // 2
    state_spec = P(('inst', 'qx', 'qy'))
    vmem = pl.BlockSpec(memory_space=pltpu.VMEM)
    smem = pl.BlockSpec(memory_space=pltpu.SMEM)
    hbm = pl.BlockSpec(memory_space=pl.ANY)

    def device_body(cost_loc, gamma_angles, beta_angles):
        local = cost_loc.shape[0]
        rows = local // LANES
        total_bits = int(math.log2(local * nqx * nqy))
        layers = gamma_angles.shape[0]
        st = jax.ShapeDtypeStruct((rows, LANES), F32)
        state = pltpu.VMEM((2, 4, LANES, LANES), F32)
        weights = pltpu.VMEM((layers, 3, 2 * LANES, 2 * LANES), BF16)
        energy, re, im = pl.pallas_call(
            functools.partial(kernel, layers, total_bits, half, nqy),
            out_shape=(jax.ShapeDtypeStruct((1,), F32), st, st),
            in_specs=[smem, smem, hbm], out_specs=(smem, vmem, vmem),
            scratch_shapes=[pltpu.VMEM((rows, LANES), F32), pltpu.VMEM((half, 8, LANES), F32), pltpu.VMEM((8, LANES), F32),
                            state, state, state, weights, weights,
                            pltpu.SemaphoreType.DMA, pltpu.SemaphoreType.DMA((half,)), pltpu.SemaphoreType.DMA((half,))],
            compiler_params=pltpu.CompilerParams(collective_id=0, has_side_effects=True),
        )(gamma_angles, beta_angles, cost_loc.reshape(rows, LANES))
        return energy, re.reshape(local), im.reshape(local)

    return jax.shard_map(device_body, mesh=mesh, in_specs=(state_spec, P(), P()), out_specs=(P('inst'), state_spec, state_spec), check_vma=False)
```

```python
import functools
import math
import jax
import jax.numpy as jnp
from jax import lax
from jax.experimental import pallas as pl
from jax.experimental.pallas import tpu as pltpu
from jax.sharding import PartitionSpec as P

LANES = 128
SIN_POLY = (4.442883014678955, -7.308245658874512, 3.606354236602783, -0.8461116552352905, 0.1098245158791542)
COS_POLY = (1.4142135381698608, -6.9788641929626465, 5.73988151550293, -1.888274908065796, 0.33225154876708984, -0.034501612186431885)
F32 = jnp.float32
BF16 = jnp.bfloat16


def flip_bits(value, mask):
    bit = 1
    while bit <= mask:
        if mask & bit:
            value = value + bit * (1 - 2 * ((value // bit) % 2))
        bit *= 2
    return value


def turn_cos_sin(turns):
    rem = turns - jnp.round(turns)
    sq = rem * rem
    s = SIN_POLY[-1]
    for k in SIN_POLY[-2::-1]:
        s = s * sq + k
    s = s * rem
    c = COS_POLY[-1]
    for k in COS_POLY[-2::-1]:
        c = c * sq + k
    return 1.0 - s * s, s * c


def split3(x):
    a = x.astype(BF16)
    r = x - a.astype(F32)
    b = r.astype(BF16)
    c = (r - b.astype(F32)).astype(BF16)
    return a, b, c


def dot6_lhs(lhs_parts, rhs_cat):
    a, b, c = lhs_parts
    return jnp.dot(jnp.concatenate([a, a, b, a, b, c], axis=1), rhs_cat, preferred_element_type=F32)


def reverse_rows(x):
    n = x.shape[0]
    i = lax.broadcasted_iota(jnp.int32, (n, n), 0)
    j = lax.broadcasted_iota(jnp.int32, (n, n), 1)
    perm = jnp.where(i + j == n - 1, 1.0, 0.0).astype(F32)
    return jnp.dot(perm, x, precision=lax.Precision.HIGHEST, preferred_element_type=F32)


def product_matrix(diag, off0, off1, scale):
    lane = lax.broadcasted_iota(jnp.int32, (8, LANES), 1)
    sub = lax.broadcasted_iota(jnp.int32, (8, LANES), 0)
    bit = lambda v, b: (v // (1 << b)) % 2
    base = jnp.full((8, LANES), 1.0, F32) * scale
    rows = [[None, None] for _ in range(7)]
    for b in range(7):
        lb = bit(lane, b) == 1
        row0 = jnp.where(lb, off0, diag[0])
        row1 = jnp.where(lb, diag[1], off1)
        rows[b] = [row0, row1]
    for b in range(3):
        base = base * jnp.where(bit(sub, b) == 1, rows[b][1], rows[b][0])
    blocks = [base]
    for b in range(3, 7):
        blocks = [x * rows[b][0] for x in blocks] + [x * rows[b][1] for x in blocks]
    return jnp.concatenate(blocks, axis=0)


def kernel(layers, total_bits, half, nqy, gamma_hbm, beta_hbm, cost_hbm, energy_ref, re_ref, im_ref,
           cost_ref, table_ref, packet, cst, sre, sim, wcat_ref, mcat_ref, gamma_ref, beta_ref, load_sem, angle_sem, send_sem, recv_sem):
    load = pltpu.make_async_copy(cost_hbm, cost_ref, load_sem)
    load.start()
    angle_loads = [pltpu.make_async_copy(gamma_hbm, gamma_ref, angle_sem.at[0]),
                   pltpu.make_async_copy(beta_hbm, beta_ref, angle_sem.at[1])]
    for angle_load in angle_loads:
        angle_load.start()
    me_x, me_y = lax.axis_index('qx'), lax.axis_index('qy')
    barrier = pltpu.get_barrier_semaphore()

    def partner(e):
        return {'qx': flip_bits(me_x, e // nqy), 'qy': flip_bits(me_y, e % nqy)}

    for e in range(1, half):
        pl.semaphore_signal(barrier, inc=1, device_id=partner(e), device_id_type=pl.DeviceIdType.MESH)
    load.wait()
    rows = cost_ref.shape[0]
    cost = cost_ref[...]
    rev = reverse_rows(cost)
    col = jnp.concatenate([cost, rev], axis=0).T[0:1, :]
    packet[0:1, :] = cost[0:1, :]
    packet[1:2, :] = col
    pl.semaphore_wait(barrier, half - 1)
    copies = []
    for e in range(1, half):
        copy = pltpu.make_async_remote_copy(
            src_ref=packet.at[0:2], dst_ref=table_ref.at[e, 0:2], send_sem=send_sem.at[e], recv_sem=recv_sem.at[e],
            device_id=partner(e), device_id_type=pl.DeviceIdType.MESH)
        copy.start()
        copies.append(copy)
    for angle_load in angle_loads:
        angle_load.wait()
    trig = []
    for l in range(layers):
        half_beta = jnp.full((8, LANES), 0.5, F32) * beta_ref[l]
        c, s = jnp.cos(half_beta), jnp.sin(half_beta)
        rot = product_matrix((c, c), -s, s, c)
        rot_t = product_matrix((c, c), s, -s, c)
        rk = product_matrix((-s, -s), -c, c, -s)
        rk_t = product_matrix((-s, -s), c, -c, -s)
        w = jnp.concatenate([jnp.concatenate([rot, rk], axis=1), jnp.concatenate([rk, rot], axis=1)], axis=0)
        m = jnp.concatenate([jnp.concatenate([rot_t, rk_t], axis=1), jnp.concatenate([rk_t, rot_t], axis=1)], axis=0)
        for k, part in enumerate(split3(w)):
            wcat_ref[l, k] = part
        for k, part in enumerate(split3(m)):
            mcat_ref[l, k] = part
        trig.append(((c * c)[0:1, :], (s * s)[0:1, :], (s * c)[0:1, :]))

    lane = lax.broadcasted_iota(jnp.int32, (LANES, LANES), 1)
    vrow = lax.broadcasted_iota(jnp.int32, (LANES, LANES), 0)
    ones = jnp.zeros((LANES, LANES), jnp.int32)
    for b in range(7):
        ones = ones + (lane // (1 << b)) % 2 + (vrow // (1 << b)) % 2
    quarter = (ones % 4).astype(F32) * 0.25

    for copy in copies:
        copy.wait()
    first = jnp.concatenate([(table_ref[e, 0:1, :] - cost[0:1, :]) if e else jnp.zeros((1, LANES), F32) for e in range(16)], axis=0)
    own_col = col
    cols = jnp.concatenate([(table_ref[e, 1:2, :] - own_col) if e else jnp.zeros((1, LANES), F32) for e in range(16)], axis=0)
    cols = cols - cols[:, 0:1]
    cols_t = jnp.concatenate([cols, jnp.zeros((LANES - 16, LANES), F32)], axis=0).T
    for t in range(2):
        for u in range(4):
            for e0s in range(2):
                e = t * 8 + u * 2 + (e0s ^ t)
                base = rev if t else cost
                cst[t, u, e0s * rows:(e0s + 1) * rows, :] = base + (first[e:e + 1, :] + cols_t[t * rows:(t + 1) * rows, e:e + 1])

    amp = 2.0 ** (-total_bits / 2.0)
    for l in range(layers):
        g = gamma_ref[l] * (1.0 / (2.0 * math.pi))
        w1, w2, w3 = [wcat_ref[l, k] for k in range(3)]
        wcat = jnp.concatenate([w1, w1, w2, w1, w2, w3], axis=1)
        m1, m2, m3 = [mcat_ref[l, k] for k in range(3)]
        mcat = jnp.concatenate([m1, m2, m1, m3, m2, m1], axis=0)
        c2, s2, sc = trig[l]
        ys = []
        for u in range(4):
            parts = []
            for t in range(2):
                turns = cst[t, u] * g
                if l == 0:
                    turns = turns - jnp.round(turns) - quarter
                    co, si = turn_cos_sin(turns)
                    re, im = amp * co, -amp * si
                else:
                    co, si = turn_cos_sin(turns)
                    a, b = sre[t, u], sim[t, u]
                    re, im = a * co + b * si, b * co - a * si
                parts.append(jnp.concatenate([re, im], axis=1))
            x1, x2, x3 = split3(jnp.concatenate(parts, axis=0))
            xcat = jnp.concatenate([x1, x2, x1, x3, x2, x1], axis=0)
            ys.append(jnp.dot(wcat, xcat, preferred_element_type=F32))
        zs = {}
        for u in range(4):
            y0, y1 = ys[u], ys[3 - u]
            lhs = jnp.concatenate([
                jnp.concatenate([y0[:LANES, :LANES], y1[LANES:, :LANES]], axis=1),
                jnp.concatenate([y0[:LANES, LANES:], y1[LANES:, LANES:]], axis=1)], axis=0)
            z = dot6_lhs(split3(lhs), mcat)
            zs[0, u] = (z[:LANES, :LANES], z[LANES:, :LANES])
            zs[1, 3 - u] = (z[:LANES, LANES:], z[LANES:, LANES:])
        for t in range(2):
            zr = [zs[t, u][0] for u in range(4)]
            zi = [zs[t, u][1] for u in range(4)]
            br = [sc * (zi[1] + zi[2]), sc * (zi[0] + zi[3])]
            bi = [sc * (zr[1] + zr[2]), sc * (zr[0] + zr[3])]
            for u in range(4):
                k = 0 if u in (0, 3) else 1
                sre[t, u] = c2 * zr[u] - s2 * zr[3 - u] + br[k]
                sim[t, u] = c2 * zi[u] - s2 * zi[3 - u] - bi[k]

    total = jnp.zeros((LANES, LANES), F32)
    for t in range(2):
        for u in range(4):
            a, b = sre[t, u], sim[t, u]
            total = total + cst[t, u] * (a * a + b * b)
    energy_ref[...] = jnp.sum(total.reshape(16, 8, LANES), axis=0)
    a, b = sre[0, 0, 0:rows, :], sim[0, 0, 0:rows, :]
    k = ones[0:rows, :] % 4
    re_ref[...] = jnp.where(k == 0, a, jnp.where(k == 1, b, jnp.where(k == 2, -a, -b)))
    im_ref[...] = jnp.where(k == 0, b, jnp.where(k == 1, -a, jnp.where(k == 2, -b, a)))


def write_kernel(partial_ref, re_in, im_in, energy_ref, re_ref, im_ref):
    re_ref[...] = re_in[...]
    im_ref[...] = im_in[...]
    energy_ref[0] = 2.0 * jnp.sum(partial_ref[...])


def solution(mesh):
    nqx, nqy = mesh.shape['qx'], mesh.shape['qy']
    half = nqx * nqy // 2
    state_spec = P(('inst', 'qx', 'qy'))
    vmem = pl.BlockSpec(memory_space=pltpu.VMEM)
    smem = pl.BlockSpec(memory_space=pltpu.SMEM)
    hbm = pl.BlockSpec(memory_space=pltpu.HBM)

    def device_body(cost_loc, gamma_angles, beta_angles):
        local = cost_loc.shape[0]
        rows = local // LANES
        total_bits = int(math.log2(local * nqx * nqy))
        layers = gamma_angles.shape[0]
        st = jax.ShapeDtypeStruct((rows, LANES), F32)
        state = pltpu.VMEM((2, 4, LANES, LANES), F32)
        weights = pltpu.VMEM((layers, 3, 2 * LANES, 2 * LANES), BF16)
        partial, re, im = pl.pallas_call(
            functools.partial(kernel, layers, total_bits, half, nqy),
            out_shape=(jax.ShapeDtypeStruct((8, LANES), F32), st, st),
            in_specs=[hbm, hbm, hbm], out_specs=(vmem, vmem, vmem),
            scratch_shapes=[pltpu.VMEM((rows, LANES), F32), pltpu.VMEM((half, 8, LANES), F32), pltpu.VMEM((8, LANES), F32),
                            state, state, state, weights, weights,
                            pltpu.SMEM(gamma_angles.shape, F32), pltpu.SMEM(beta_angles.shape, F32),
                            pltpu.SemaphoreType.DMA, pltpu.SemaphoreType.DMA((2,)),
                            pltpu.SemaphoreType.DMA((half,)), pltpu.SemaphoreType.DMA((half,))],
            compiler_params=pltpu.CompilerParams(collective_id=0, has_side_effects=True, vmem_limit_bytes=32 * 1024 * 1024),
        )(*[pltpu.with_memory_space_constraint(x, pltpu.HBM) for x in (gamma_angles, beta_angles, cost_loc.reshape(rows, LANES))])
        energy, re, im = pl.pallas_call(
            write_kernel, out_shape=(jax.ShapeDtypeStruct((1,), F32), st, st),
            in_specs=[vmem, vmem, vmem], out_specs=(smem, vmem, vmem),
            compiler_params=pltpu.CompilerParams(vmem_limit_bytes=4 * 1024 * 1024),
        )(partial, re, im)
        return energy, re.reshape(local), im.reshape(local)

    return jax.shard_map(device_body, mesh=mesh, in_specs=(state_spec, P(), P()), out_specs=(P('inst'), state_spec, state_spec), check_vma=False)
```

```python
import functools
import math
import jax
import jax.numpy as jnp
from jax import lax
from jax.experimental import pallas as pl
from jax.experimental.pallas import tpu as pltpu
from jax.sharding import PartitionSpec as P

LANES = 128
SIN_POLY = (4.442883014678955, -7.308245658874512, 3.606354236602783, -0.8461116552352905, 0.1098245158791542)
COS_POLY = (1.4142135381698608, -6.9788641929626465, 5.73988151550293, -1.888274908065796, 0.33225154876708984, -0.034501612186431885)
F32 = jnp.float32
BF16 = jnp.bfloat16


def flip_bits(value, mask):
    bit = 1
    while bit <= mask:
        if mask & bit:
            value = value + bit * (1 - 2 * ((value // bit) % 2))
        bit *= 2
    return value


def turn_cos_sin(turns):
    rem = turns - jnp.round(turns)
    sq = rem * rem
    s = SIN_POLY[-1]
    for k in SIN_POLY[-2::-1]:
        s = s * sq + k
    s = s * rem
    c = COS_POLY[-1]
    for k in COS_POLY[-2::-1]:
        c = c * sq + k
    return 1.0 - s * s, s * c


def split3(x):
    a = x.astype(BF16)
    r = x - a.astype(F32)
    b = r.astype(BF16)
    c = (r - b.astype(F32)).astype(BF16)
    return a, b, c


def reverse_rows(x):
    n = x.shape[0]
    i = lax.broadcasted_iota(jnp.int32, (n, n), 0)
    j = lax.broadcasted_iota(jnp.int32, (n, n), 1)
    perm = jnp.where(i + j == n - 1, 1.0, 0.0).astype(F32)
    return jnp.dot(perm, x, precision=lax.Precision.HIGHEST, preferred_element_type=F32)


def product_matrix(diag, off0, off1, scale):
    lane = lax.broadcasted_iota(jnp.int32, (8, LANES), 1)
    sub = lax.broadcasted_iota(jnp.int32, (8, LANES), 0)
    bit = lambda v, b: (v // (1 << b)) % 2
    base = jnp.full((8, LANES), 1.0, F32) * scale
    rows = [[None, None] for _ in range(7)]
    for b in range(7):
        lb = bit(lane, b) == 1
        row0 = jnp.where(lb, off0, diag[0])
        row1 = jnp.where(lb, diag[1], off1)
        rows[b] = [row0, row1]
    for b in range(3):
        base = base * jnp.where(bit(sub, b) == 1, rows[b][1], rows[b][0])
    blocks = [base]
    for b in range(3, 7):
        blocks = [x * rows[b][0] for x in blocks] + [x * rows[b][1] for x in blocks]
    return jnp.concatenate(blocks, axis=0)


CHUNKS = 4


def kernel(layers, total_bits, half, nqy, gamma_hbm, beta_hbm, cost_hbm, energy_ref, re_ref, im_ref,
           cost_ref, table_ref, packet, cst, base_ref, start_ref, low_ref, high_ref, ph_ref, sx, lx, w_ref, h_ref, trig_ref, gamma_ref, beta_ref,
           load_sem, angle_sem, send_sem, recv_sem):
    load = pltpu.make_async_copy(cost_hbm, cost_ref, load_sem)
    load.start()
    angle_loads = [pltpu.make_async_copy(gamma_hbm, gamma_ref, angle_sem.at[0]),
                   pltpu.make_async_copy(beta_hbm, beta_ref, angle_sem.at[1])]
    for angle_load in angle_loads:
        angle_load.start()
    me_x, me_y = lax.axis_index('qx'), lax.axis_index('qy')
    barrier = pltpu.get_barrier_semaphore()
    partners = {e: {'qx': flip_bits(me_x, e // nqy), 'qy': flip_bits(me_y, e % nqy)} for e in range(1, half)}
    order = sorted(range(1, half), key=lambda e: (-(e // (2 * nqy)) - (0, 1, 2, 1)[e % nqy], e))
    for e in order:
        pl.semaphore_signal(barrier, inc=1, device_id=partners[e], device_id_type=pl.DeviceIdType.MESH)
    load.wait()
    rows = cost_ref.shape[0]
    row_bits = int(math.log2(rows))
    lane1 = lax.broadcasted_iota(jnp.int32, (1, LANES), 1)
    slopes = jnp.zeros((1, LANES), F32)
    for k in range(row_bits):
        row = cost_ref[(1 << k):(1 << k) + 1, :]
        slopes = jnp.where(lane1 == k, row if k == 0 else pltpu.roll(row, k, axis=1), slopes)
    packet[0:1, :] = cost_ref[0:1, :]
    packet[1:2, :] = slopes
    pl.semaphore_wait(barrier, half - 1)
    copies = {}
    for e in order:
        copies[e] = pltpu.make_async_remote_copy(
            src_ref=packet.at[0:2], dst_ref=table_ref.at[e, 0:2], send_sem=send_sem.at[e], recv_sem=recv_sem.at[e],
            device_id=partners[e], device_id_type=pl.DeviceIdType.MESH)
        copies[e].start()
    for angle_load in angle_loads:
        angle_load.wait()
    zero = jnp.zeros((LANES, LANES), BF16)
    for l in range(layers):
        half_beta = jnp.full((8, LANES), 0.5, F32) * beta_ref[l]
        c, s = jnp.cos(half_beta), jnp.sin(half_beta)
        a = product_matrix((c, c), -s, s, 0.5 * c)
        b = product_matrix((-s, -s), -c, c, -0.5 * s)
        a_t = product_matrix((c, c), s, -s, 0.25 * c)
        b_t = product_matrix((-s, -s), c, -c, -0.25 * s)
        for pq in range(2):
            g1, g2, g3 = split3(a - b if pq else a + b)
            w_ref[l, pq] = jnp.concatenate([jnp.concatenate([g1, g1, g1, zero], axis=1),
                                            jnp.concatenate([g2, g2, zero, g3], axis=1)], axis=0)
            h1, h2, h3 = split3(a_t - b_t if pq else a_t + b_t)
            h_ref[l, pq] = jnp.concatenate([jnp.concatenate([h1, h1, h1, zero], axis=0),
                                            jnp.concatenate([h2, h2, zero, h3], axis=0)], axis=1)
        trig_ref[l, 0] = c * c - s * s
        trig_ref[l, 1] = 2.0 * (s * c)

    lane = lax.broadcasted_iota(jnp.int32, (LANES, LANES), 1)
    vrow = lax.broadcasted_iota(jnp.int32, (LANES, LANES), 0)
    ones = jnp.zeros((LANES, LANES), jnp.int32)
    for b in range(7):
        ones = ones + (lane // (1 << b)) % 2 + (vrow // (1 << b)) % 2
    ones = ones % 4
    quarter = ones.astype(F32) * 0.25
    amp = 2.0 ** (-total_bits / 2.0)
    cost = cost_ref[...]
    bases = (cost, reverse_rows(cost))
    sub = lax.broadcasted_iota(jnp.int32, (8, LANES), 0)

    def unit(turns):
        co, si = turn_cos_sin(turns)
        return co, -si

    def mul(x, y):
        return x[0] * y[0] - x[1] * y[1], x[0] * y[1] + x[1] * y[0]

    rates = [gamma_ref[l] * (1.0 / (2.0 * math.pi)) for l in range(layers)]
    for t in range(2):
        for l in range(1, layers):
            for i, x in enumerate(unit(bases[t] * rates[l])):
                base_ref[l, t, i] = x
        turns = bases[t] * rates[0]
        turns = turns - jnp.round(turns) - quarter[:rows]
        re, im = unit(turns)
        re, im = amp * re, amp * im
        for e0s, pair in enumerate(((re, im), (-im, re))):
            for i, x in enumerate(pair):
                start_ref[t, e0s, i] = x

    def place(e):
        t = e // (2 * nqy)
        return t, e % nqy, (e // nqy) % 2 ^ t

    def put_state(u, lo, x0, x1):
        n = x0.shape[0]
        for pq, x in enumerate((x0 + x1, x0 - x1)):
            for k, part in enumerate(split3(x)):
                sx[u, pq, k, lo:lo + n, :] = part

    def rows_stage(l, u):
        out = []
        for pq in range(2):
            x = [sx[u, pq, k] for k in range(3)]
            y = jnp.dot(w_ref[l, pq], jnp.concatenate(x + x[:1], axis=0), preferred_element_type=F32)
            out.append(y[:LANES] + y[LANES:])
        return out

    def put_pair(u, ys):
        step = LANES // CHUNKS
        for a, b in ((u, 3 - u), (3 - u, u)):
            y0 = ys[a][0] + ys[a][1]
            y1 = ys[b][0] - ys[b][1]
            for pq, y in enumerate((y0 + y1, y0 - y1)):
                for k, part in enumerate(split3(y)):
                    for j in range(CHUNKS):
                        for i in range(2):
                            lo = (a * 2 + i) * step
                            lx[j, pq, k, lo:lo + step, :] = part[j * step:(j + 1) * step, i * LANES:(i + 1) * LANES]

    def lanes_stage(l, j):
        cb, sb = trig_ref[l, 0, 0:1, :], trig_ref[l, 1, 0:1, :]
        step = LANES // CHUNKS
        psi = []
        for pq in range(2):
            x = [lx[j, pq, k] for k in range(3)]
            z = jnp.dot(jnp.concatenate(x + x[:1], axis=1), h_ref[l, pq], preferred_element_type=F32)
            z = z[:, :LANES] + z[:, LANES:]
            f = [[z[(u * 2 + i) * step:(u * 2 + i + 1) * step] for i in range(2)] for u in range(4)]
            p = [f[0][i] + f[3][i] for i in range(2)]
            m = [f[0][i] - f[3][i] for i in range(2)]
            q = [f[1][i] + f[2][i] for i in range(2)]
            n = [f[1][i] - f[2][i] for i in range(2)]
            p, q = ((cb * p[0] + sb * q[1], cb * p[1] - sb * q[0]), (cb * q[0] + sb * p[1], cb * q[1] - sb * p[0]))
            psi.append([[p[i] + m[i] for i in range(2)], [q[i] + n[i] for i in range(2)],
                        [q[i] - n[i] for i in range(2)], [p[i] - m[i] for i in range(2)]])
        first = [[psi[0][u][i] + psi[1][u][i] for i in range(2)] for u in range(4)]
        second = [[psi[0][3 - u][i] - psi[1][3 - u][i] for i in range(2)] for u in range(4)]
        return first, second

    for e in order:
        copies[e].wait()
    first = jnp.concatenate([(table_ref[e, 0:1, :] - cost[0:1, :]) if e else jnp.zeros((1, LANES), F32) for e in range(half)], axis=0)
    slope = jnp.concatenate([(table_ref[e, 1:2, :] - slopes) if e else jnp.zeros((1, LANES), F32) for e in range(half)], axis=0)
    slope = slope - first[:, 0:1]
    cols = [jnp.broadcast_to(slope[:, k:k + 1], (half, LANES)) for k in range(row_bits)]
    low = {}
    for e in range(1, half):
        part = jnp.broadcast_to(first[e:e + 1, :], (8, LANES))
        for k in range(3):
            part = part + jnp.where((sub // (1 << k)) % 2 == 1 - e // (2 * nqy), cols[k][e:e + 1, :], 0.0)
        low[e] = part

    def put_factors(l):
        for k in range(3, row_bits):
            for i, x in enumerate(unit(cols[k] * rates[l])):
                high_ref[l, k - 3, i] = x
        for e in range(1, half):
            for i, x in enumerate(unit(low[e] * rates[l])):
                low_ref[l, e, i] = x

    def factors(l, e):
        out = [(low_ref[l, e, 0], low_ref[l, e, 1])]
        for k in range(row_bits - 3):
            h = (high_ref[l, k, 0, e:e + 1, :], high_ref[l, k, 1, e:e + 1, :])
            more = [mul(x, h) for x in out]
            out = more + out if e // (2 * nqy) else out + more
        return [jnp.concatenate([x[i] for x in out], axis=0) for i in range(2)]

    def put_phases(l, us):
        for e in range(half):
            t, u, e0s = place(e)
            if u in us:
                x = (base_ref[l, t, 0], base_ref[l, t, 1])
                if e:
                    x = mul(x, factors(l, e))
                for i in range(2):
                    ph_ref[t, u, i, e0s * rows:(e0s + 1) * rows, :] = x[i]

    def put_cost(us):
        for e in range(half):
            t, u, e0s = place(e)
            if u in us:
                block = bases[t]
                if e:
                    parts = [low[e]]
                    for k in range(3, row_bits):
                        more = [x + cols[k][e:e + 1, :] for x in parts]
                        parts = more + parts if t else parts + more
                    block = block + jnp.concatenate(parts, axis=0)
                cst[t, u, e0s * rows:(e0s + 1) * rows, :] = block

    put_factors(0)
    ys = {}
    for u in (0, 3, 1, 2):
        xs = [[None, None], [None, None]]
        for e in range(half):
            if e % nqy == u:
                t, _, e0s = place(e)
                x = (start_ref[t, e0s, 0], start_ref[t, e0s, 1])
                xs[t][e0s] = jnp.concatenate(mul(x, factors(0, e)) if e else x, axis=1)
        put_state(u, 0, *[jnp.concatenate(x, axis=0) for x in xs])
        ys[u] = rows_stage(0, u)
        if u == 3:
            put_pair(0, ys)
        if u == 2:
            put_pair(1, ys)
    put_factors(1)
    put_phases(1, range(nqy))

    step = LANES // CHUNKS
    total = jnp.zeros((8, LANES), F32)
    for l in range(layers):
        for j in range(CHUNKS):
            both = lanes_stage(l, j)
            at = pl.ds(j * step, step)
            if l < layers - 1:
                for u in range(4):
                    xs = []
                    for t in range(2):
                        a, b = both[t][u]
                        pr, pi = ph_ref[t, u, 0, at, :], ph_ref[t, u, 1, at, :]
                        xs.append(jnp.concatenate([a * pr - b * pi, b * pr + a * pi], axis=1))
                    put_state(u, j * step, *xs)
            else:
                for u in range(4):
                    for t in range(2):
                        a, b = both[t][u]
                        total = total + jnp.sum((cst[t, u, at, :] * (a * a + b * b)).reshape(step // 8, 8, LANES), axis=0)
                if j * step < rows:
                    a, b = both[0][0]
                    k = ones[j * step:(j + 1) * step, :]
                    re_ref[at, :] = jnp.where(k == 0, a, jnp.where(k == 1, b, jnp.where(k == 2, -a, -b)))
                    im_ref[at, :] = jnp.where(k == 0, b, jnp.where(k == 1, -a, jnp.where(k == 2, -b, a)))
        if l < layers - 1:
            ys = {}
            for u in (0, 3, 1, 2):
                ys[u] = rows_stage(l + 1, u)
                if u == 3:
                    put_pair(0, ys)
                if u == 2:
                    put_pair(1, ys)
            if l + 2 < layers:
                put_factors(l + 2)
                put_phases(l + 2, range(nqy))
            else:
                put_cost(range(nqy))
    energy_ref[...] = total


def write_kernel(partial_ref, re_in, im_in, energy_ref, re_ref, im_ref):
    re_ref[...] = re_in[...]
    im_ref[...] = im_in[...]
    energy_ref[0] = 2.0 * jnp.sum(partial_ref[...])


def solution(mesh):
    nqx, nqy = mesh.shape['qx'], mesh.shape['qy']
    half = nqx * nqy // 2
    state_spec = P(('inst', 'qx', 'qy'))
    vmem = pl.BlockSpec(memory_space=pltpu.VMEM)
    smem = pl.BlockSpec(memory_space=pltpu.SMEM)
    hbm = pl.BlockSpec(memory_space=pltpu.HBM)

    def device_body(cost_loc, gamma_angles, beta_angles):
        local = cost_loc.shape[0]
        rows = local // LANES
        total_bits = int(math.log2(local * nqx * nqy))
        layers = gamma_angles.shape[0]
        st = jax.ShapeDtypeStruct((rows, LANES), F32)
        partial, re, im = pl.pallas_call(
            functools.partial(kernel, layers, total_bits, half, nqy),
            out_shape=(jax.ShapeDtypeStruct((8, LANES), F32), st, st),
            in_specs=[hbm, hbm, hbm], out_specs=(vmem, vmem, vmem),
            scratch_shapes=[pltpu.VMEM((rows, LANES), F32), pltpu.VMEM((half, 8, LANES), F32), pltpu.VMEM((8, LANES), F32),
                            pltpu.VMEM((2, 4, LANES, LANES), F32),
                            pltpu.VMEM((layers, 2, 2, rows, LANES), F32), pltpu.VMEM((2, 2, 2, rows, LANES), F32),
                            pltpu.VMEM((layers, half, 2, 8, LANES), F32), pltpu.VMEM((layers, 3, 2, half, LANES), F32),
                            pltpu.VMEM((2, 4, 2, LANES, LANES), F32),
                            pltpu.VMEM((4, 2, 3, LANES, 2 * LANES), BF16), pltpu.VMEM((CHUNKS, 2, 3, 8 * LANES // CHUNKS, LANES), BF16),
                            pltpu.VMEM((layers, 2, 2 * LANES, 4 * LANES), BF16), pltpu.VMEM((layers, 2, 4 * LANES, 2 * LANES), BF16),
                            pltpu.VMEM((layers, 2, 8, LANES), F32),
                            pltpu.SMEM(gamma_angles.shape, F32), pltpu.SMEM(beta_angles.shape, F32),
                            pltpu.SemaphoreType.DMA, pltpu.SemaphoreType.DMA((2,)),
                            pltpu.SemaphoreType.DMA((half,)), pltpu.SemaphoreType.DMA((half,))],
            compiler_params=pltpu.CompilerParams(collective_id=0, has_side_effects=True, vmem_limit_bytes=32 * 1024 * 1024),
        )(*[pltpu.with_memory_space_constraint(x, pltpu.HBM) for x in (gamma_angles, beta_angles, cost_loc.reshape(rows, LANES))])
        energy, re, im = pl.pallas_call(
            write_kernel, out_shape=(jax.ShapeDtypeStruct((1,), F32), st, st),
            in_specs=[vmem, vmem, vmem], out_specs=(smem, vmem, vmem),
            compiler_params=pltpu.CompilerParams(vmem_limit_bytes=4 * 1024 * 1024),
        )(partial, re, im)
        return energy, re.reshape(local), im.reshape(local)

    return jax.shard_map(device_body, mesh=mesh, in_specs=(state_spec, P(), P()), out_specs=(P('inst'), state_spec, state_spec), check_vma=False)
```

```python
import functools
import math
import jax
import jax.numpy as jnp
from jax import lax
from jax.experimental import pallas as pl
from jax.experimental.pallas import tpu as pltpu
from jax.sharding import PartitionSpec as P

LANES = 128
QUAD = 4
SIN_POLY = (4.442883014678955, -7.308245658874512, 3.606354236602783, -0.8461116552352905, 0.1098245158791542)
COS_POLY = (1.4142135381698608, -6.9788641929626465, 5.73988151550293, -1.888274908065796, 0.33225154876708984, -0.034501612186431885)
F32 = jnp.float32
BF16 = jnp.bfloat16


def flip_bits(value, mask):
    bit = 1
    while bit <= mask:
        if mask & bit:
            value = value + bit * (1 - 2 * ((value // bit) % 2))
        bit *= 2
    return value


def turn_cos_sin(turns):
    rem = turns - jnp.round(turns)
    sq = rem * rem
    s = SIN_POLY[-1]
    for k in SIN_POLY[-2::-1]:
        s = s * sq + k
    s = s * rem
    c = COS_POLY[-1]
    for k in COS_POLY[-2::-1]:
        c = c * sq + k
    return 1.0 - s * s, s * c


def split3(x):
    a = x.astype(BF16)
    r = x - a.astype(F32)
    b = r.astype(BF16)
    c = (r - b.astype(F32)).astype(BF16)
    return a, b, c


def missing(diff, e):
    bits = [1 << b for b in range(e.bit_length()) if e >> b & 1]
    if len(bits) == 2:
        a, b = bits
        c = next(1 << k for k in range(4) if not e >> k & 1 and all(x in diff for x in (e | 1 << k, a | 1 << k, b | 1 << k)))
        return diff[e | c] - diff[a | c] - diff[b | c] + diff[a] + diff[b] + diff[c]
    pairs = [a | b for i, a in enumerate(bits) for b in bits[:i]]
    total = diff[pairs[0]]
    for p in pairs[1:]:
        total = total + diff[p]
    return total - (len(bits) - 2.0) * sum((diff[b] for b in bits[1:]), diff[bits[0]])


def reverse_rows(x):
    n = x.shape[0]
    i = lax.broadcasted_iota(jnp.int32, (n, n), 0)
    j = lax.broadcasted_iota(jnp.int32, (n, n), 1)
    perm = jnp.where(i + j == n - 1, 1.0, 0.0).astype(F32)
    return jnp.dot(perm, x, precision=lax.Precision.HIGHEST, preferred_element_type=F32)


def product_matrix(diag, off0, off1, scale):
    lane = lax.broadcasted_iota(jnp.int32, (8, LANES), 1)
    sub = lax.broadcasted_iota(jnp.int32, (8, LANES), 0)
    bit = lambda v, b: (v // (1 << b)) % 2
    base = jnp.full((8, LANES), 1.0, F32) * scale
    rows = [[None, None] for _ in range(7)]
    for b in range(7):
        lb = bit(lane, b) == 1
        row0 = jnp.where(lb, off0, diag[0])
        row1 = jnp.where(lb, diag[1], off1)
        rows[b] = [row0, row1]
    for b in range(3):
        base = base * jnp.where(bit(sub, b) == 1, rows[b][1], rows[b][0])
    blocks = [base]
    for b in range(3, 7):
        blocks = [x * rows[b][0] for x in blocks] + [x * rows[b][1] for x in blocks]
    return jnp.concatenate(blocks, axis=0)


CHUNKS = ((0, 32), (32, 32), (64, 32), (96, 32))


def kernel(layers, total_bits, half, nqy, gamma_hbm, beta_hbm, cost_hbm, energy_ref, re_ref, im_ref,
           cost_ref, table_ref, diff_ref, packet, cst, base_ref, start_ref, low_ref, high_ref, ph_ref, sx, lx, w_ref, h_ref, trig_ref, gamma_ref, beta_ref,
           load_sem, angle_sem, send_sem, recv_sem):
    load = pltpu.make_async_copy(cost_hbm, cost_ref, load_sem)
    load.start()
    angle_loads = [pltpu.make_async_copy(gamma_hbm, gamma_ref, angle_sem.at[0]),
                   pltpu.make_async_copy(beta_hbm, beta_ref, angle_sem.at[1])]
    for angle_load in angle_loads:
        angle_load.start()
    me_x, me_y = lax.axis_index('qx'), lax.axis_index('qy')
    barrier = pltpu.get_barrier_semaphore()
    near = nqy // 2
    hops = {e: (0, 1, 2, 1)[e // (2 * near)] + e % near for e in range(1, half)}
    asked = [e for e in hops if hops[e] < 2 or (hops[e] == 2 and (e // near) % 2 == 0)]
    order = sorted(asked, key=lambda e: (-hops[e], e))
    partners = {e: {'qx': flip_bits(me_x, e // near), 'qy': flip_bits(me_y, e % near)} for e in order}
    for e in order:
        pl.semaphore_signal(barrier, inc=1, device_id=partners[e], device_id_type=pl.DeviceIdType.MESH)
    load.wait()
    rows = cost_ref.shape[0]
    row_bits = int(math.log2(rows))
    lane1 = lax.broadcasted_iota(jnp.int32, (1, LANES), 1)
    slopes = jnp.zeros((1, LANES), F32)
    for k in range(row_bits):
        row = cost_ref[(1 << k):(1 << k) + 1, :]
        slopes = jnp.where(lane1 == k, row if k == 0 else pltpu.roll(row, k, axis=1), slopes)
    packet[0:1, :] = cost_ref[0:1, :]
    packet[1:2, :] = slopes
    own = packet[...]
    pl.semaphore_wait(barrier, len(order))
    copies = {}
    for e in order:
        copies[e] = pltpu.make_async_remote_copy(
            src_ref=packet, dst_ref=table_ref.at[:, e], send_sem=send_sem.at[e], recv_sem=recv_sem.at[e],
            device_id=partners[e], device_id_type=pl.DeviceIdType.MESH)
        copies[e].start()
    for angle_load in angle_loads:
        angle_load.wait()
    zero = jnp.zeros((LANES, LANES), BF16)
    for l in range(layers):
        half_beta = jnp.full((8, LANES), 0.5, F32) * beta_ref[l]
        c, s = jnp.cos(half_beta), jnp.sin(half_beta)
        a = product_matrix((c, c), -s, s, 0.5 * c)
        b = product_matrix((-s, -s), -c, c, -0.5 * s)
        a_t = product_matrix((c, c), s, -s, 0.25 * c)
        b_t = product_matrix((-s, -s), c, -c, -0.25 * s)
        for pq in range(2):
            g1, g2, g3 = split3(a - b if pq else a + b)
            w_ref[l, pq] = jnp.concatenate([jnp.concatenate([g1, g1, g1, zero], axis=1),
                                            jnp.concatenate([g2, g2, zero, g3], axis=1)], axis=0)
            h1, h2, h3 = split3(a_t - b_t if pq else a_t + b_t)
            h_ref[l, pq] = jnp.concatenate([jnp.concatenate([h1, h1, h1, zero], axis=0),
                                            jnp.concatenate([h2, h2, zero, h3], axis=0)], axis=1)
        trig_ref[l, 0] = c * c - s * s
        trig_ref[l, 1] = 2.0 * (s * c)

    lane = lax.broadcasted_iota(jnp.int32, (LANES, LANES), 1)
    vrow = lax.broadcasted_iota(jnp.int32, (LANES, LANES), 0)
    ones = jnp.zeros((LANES, LANES), jnp.int32)
    for b in range(7):
        ones = ones + (lane // (1 << b)) % 2 + (vrow // (1 << b)) % 2
    ones = ones % 4
    quarter = ones.astype(F32) * 0.25
    amp = 2.0 ** (-total_bits / 2.0)
    cost = cost_ref[...]
    bases = (cost, reverse_rows(cost))
    sub = lax.broadcasted_iota(jnp.int32, (8, LANES), 0)

    def unit(turns):
        co, si = turn_cos_sin(turns)
        return co, -si

    def mul(x, y):
        return x[0] * y[0] - x[1] * y[1], x[0] * y[1] + x[1] * y[0]

    rates = [gamma_ref[l] * (1.0 / (2.0 * math.pi)) for l in range(layers)]
    for t in range(2):
        for l in range(1, layers):
            for i, x in enumerate(unit(bases[t] * rates[l])):
                base_ref[l, t, i] = x
        turns = bases[t] * rates[0]
        turns = turns - jnp.round(turns) - quarter[:rows]
        re, im = unit(turns)
        re, im = amp * re, amp * im
        for e0s, pair in enumerate(((re, im), (-im, re))):
            for i, x in enumerate(pair):
                start_ref[t, e0s, i] = x

    def place(e):
        t = e // (2 * QUAD)
        return t, e % QUAD, (e // QUAD) % 2 ^ t

    def put_state(u, lo, x0, x1):
        n = x0.shape[0]
        for pq, x in enumerate((x0 + x1, x0 - x1)):
            for k, part in enumerate(split3(x)):
                sx[u, pq, k, lo:lo + n, :] = part

    def rows_stage(l, u):
        out = []
        for pq in range(2):
            x = [sx[u, pq, k] for k in range(3)]
            y = jnp.dot(w_ref[l, pq], jnp.concatenate(x + x[:1], axis=0), preferred_element_type=F32)
            out.append(y[:LANES] + y[LANES:])
        return out

    def put_pair(u, ys):
        for a, b in ((u, 3 - u), (3 - u, u)):
            y0 = ys[a][0] + ys[a][1]
            y1 = ys[b][0] - ys[b][1]
            for pq, y in enumerate((y0 + y1, y0 - y1)):
                for k, part in enumerate(split3(y)):
                    for i in range(2):
                        lx[pq, k, a, i] = part[:, i * LANES:(i + 1) * LANES]

    def lanes_dot(l, pair, lo, n):
        out = {}
        for pq in range(2):
            x = [jnp.concatenate([lx[pq, k, u, i, lo:lo + n, :] for u in pair for i in range(2)], axis=0) for k in range(3)]
            z = jnp.dot(jnp.concatenate(x + x[:1], axis=1), h_ref[l, pq], preferred_element_type=F32)
            z = z[:, :LANES] + z[:, LANES:]
            for a, u in enumerate(pair):
                out[pq, u] = [z[(a * 2 + i) * n:(a * 2 + i + 1) * n] for i in range(2)]
        return out

    def mix_pairs(l, f):
        cb, sb = trig_ref[l, 0, 0:1, :], trig_ref[l, 1, 0:1, :]
        psi = []
        for pq in range(2):
            p = [f[pq, 0][i] + f[pq, 3][i] for i in range(2)]
            m = [f[pq, 0][i] - f[pq, 3][i] for i in range(2)]
            q = [f[pq, 1][i] + f[pq, 2][i] for i in range(2)]
            n = [f[pq, 1][i] - f[pq, 2][i] for i in range(2)]
            p, q = ((cb * p[0] + sb * q[1], cb * p[1] - sb * q[0]), (cb * q[0] + sb * p[1], cb * q[1] - sb * p[0]))
            psi.append([[p[i] + m[i] for i in range(2)], [q[i] + n[i] for i in range(2)],
                        [q[i] - n[i] for i in range(2)], [p[i] - m[i] for i in range(2)]])
        first = [[psi[0][u][i] + psi[1][u][i] for i in range(2)] for u in range(4)]
        second = [[psi[0][3 - u][i] - psi[1][3 - u][i] for i in range(2)] for u in range(4)]
        return first, second

    def lanes_stage(l):
        half_rows = LANES // 2
        early = [lanes_dot(l, (0, 3), lo, half_rows) for lo in (0, half_rows)]
        for lo, n in CHUNKS:
            f = lanes_dot(l, (1, 2), lo, n)
            at = lo % half_rows
            for key, x in early[lo // half_rows].items():
                f[key] = [y[at:at + n] for y in x]
            yield lo, n, mix_pairs(l, f)

    for e in order:
        copies[e].wait()
    diff = {0: jnp.zeros((2, LANES), F32)}
    for e in order:
        diff[e] = table_ref[:, e] - own
    for e in sorted(range(half), key=lambda e: bin(e).count('1')):
        if e not in diff:
            diff[e] = missing(diff, e)
        diff_ref[:, e] = diff[e]
    first = diff_ref[0]
    corner = jnp.broadcast_to(diff_ref[0, :, 0:1], (half, LANES))
    cols = [jnp.broadcast_to(diff_ref[1, :, k:k + 1], (half, LANES)) - corner for k in range(row_bits)]
    low = {}
    for e in range(1, half):
        part = jnp.broadcast_to(first[e:e + 1, :], (8, LANES))
        for k in range(3):
            part = part + jnp.where((sub // (1 << k)) % 2 == 1 - e // (2 * QUAD), cols[k][e:e + 1, :], 0.0)
        low[e] = part

    def put_factors(l):
        for k in range(3, row_bits):
            for i, x in enumerate(unit(cols[k] * rates[l])):
                high_ref[l, k - 3, i] = x
        for e in range(1, half):
            for i, x in enumerate(unit(low[e] * rates[l])):
                low_ref[l, e, i] = x

    def factors(l, e):
        out = [(low_ref[l, e, 0], low_ref[l, e, 1])]
        for k in range(row_bits - 3):
            h = (high_ref[l, k, 0, e:e + 1, :], high_ref[l, k, 1, e:e + 1, :])
            more = [mul(x, h) for x in out]
            out = more + out if e // (2 * QUAD) else out + more
        return [jnp.concatenate([x[i] for x in out], axis=0) for i in range(2)]

    def put_phases(l, us):
        for e in range(half):
            t, u, e0s = place(e)
            if u in us:
                x = (base_ref[l, t, 0], base_ref[l, t, 1])
                if e:
                    x = mul(x, factors(l, e))
                for i in range(2):
                    ph_ref[t, u, i, e0s * rows:(e0s + 1) * rows, :] = x[i]

    def put_cost(us):
        for e in range(half):
            t, u, e0s = place(e)
            if u in us:
                block = bases[t]
                if e:
                    parts = [low[e]]
                    for k in range(3, row_bits):
                        more = [x + cols[k][e:e + 1, :] for x in parts]
                        parts = more + parts if t else parts + more
                    block = block + jnp.concatenate(parts, axis=0)
                cst[t, u, e0s * rows:(e0s + 1) * rows, :] = block

    put_factors(0)
    ys = {}
    for u in (0, 3, 1, 2):
        xs = [[None, None], [None, None]]
        for e in range(half):
            if e % QUAD == u:
                t, _, e0s = place(e)
                x = (start_ref[t, e0s, 0], start_ref[t, e0s, 1])
                xs[t][e0s] = jnp.concatenate(mul(x, factors(0, e)) if e else x, axis=1)
        put_state(u, 0, *[jnp.concatenate(x, axis=0) for x in xs])
        ys[u] = rows_stage(0, u)
        if u == 3:
            put_pair(0, ys)
        if u == 2:
            put_pair(1, ys)
    put_factors(1)
    put_phases(1, range(QUAD))

    total = jnp.zeros((8, LANES), F32)
    for l in range(layers):
        for lo, n, both in lanes_stage(l):
            at = pl.ds(lo, n)
            if l < layers - 1:
                for u in range(4):
                    xs = []
                    for t in range(2):
                        a, b = both[t][u]
                        pr, pi = ph_ref[t, u, 0, at, :], ph_ref[t, u, 1, at, :]
                        xs.append(jnp.concatenate([a * pr - b * pi, b * pr + a * pi], axis=1))
                    put_state(u, lo, *xs)
            else:
                for u in range(4):
                    for t in range(2):
                        a, b = both[t][u]
                        total = total + jnp.sum((cst[t, u, at, :] * (a * a + b * b)).reshape(n // 8, 8, LANES), axis=0)
                if lo < rows:
                    a, b = both[0][0]
                    k = ones[lo:lo + n, :]
                    re_ref[at, :] = jnp.where(k == 0, a, jnp.where(k == 1, b, jnp.where(k == 2, -a, -b)))
                    im_ref[at, :] = jnp.where(k == 0, b, jnp.where(k == 1, -a, jnp.where(k == 2, -b, a)))
        if l < layers - 1:
            ys = {}
            for u in (0, 3, 1, 2):
                ys[u] = rows_stage(l + 1, u)
                if u == 3:
                    put_pair(0, ys)
                if u == 2:
                    put_pair(1, ys)
            if l + 2 < layers:
                put_factors(l + 2)
                put_phases(l + 2, range(QUAD))
            else:
                put_cost(range(QUAD))
    energy_ref[...] = total


def write_kernel(partial_ref, re_in, im_in, energy_ref, re_ref, im_ref):
    re_ref[...] = re_in[...]
    im_ref[...] = im_in[...]
    energy_ref[0] = 2.0 * jnp.sum(partial_ref[...])


def solution(mesh):
    nqx, nqy = mesh.shape['qx'], mesh.shape['qy']
    half = nqx * nqy // 2
    state_spec = P(('inst', 'qx', 'qy'))
    vmem = pl.BlockSpec(memory_space=pltpu.VMEM)
    smem = pl.BlockSpec(memory_space=pltpu.SMEM)
    hbm = pl.BlockSpec(memory_space=pltpu.HBM)

    def device_body(cost_loc, gamma_angles, beta_angles):
        local = cost_loc.shape[0]
        rows = local // LANES
        total_bits = int(math.log2(local * nqx * nqy))
        layers = gamma_angles.shape[0]
        st = jax.ShapeDtypeStruct((rows, LANES), F32)
        partial, re, im = pl.pallas_call(
            functools.partial(kernel, layers, total_bits, half, nqy),
            out_shape=(jax.ShapeDtypeStruct((8, LANES), F32), st, st),
            in_specs=[hbm, hbm, hbm], out_specs=(vmem, vmem, vmem),
            scratch_shapes=[pltpu.VMEM((rows, LANES), F32), pltpu.VMEM((2, half, LANES), F32), pltpu.VMEM((2, half, LANES), F32), pltpu.VMEM((2, LANES), F32),
                            pltpu.VMEM((2, 4, LANES, LANES), F32),
                            pltpu.VMEM((layers, 2, 2, rows, LANES), F32), pltpu.VMEM((2, 2, 2, rows, LANES), F32),
                            pltpu.VMEM((layers, half, 2, 8, LANES), F32), pltpu.VMEM((layers, 3, 2, half, LANES), F32),
                            pltpu.VMEM((2, 4, 2, LANES, LANES), F32),
                            pltpu.VMEM((4, 2, 3, LANES, 2 * LANES), BF16), pltpu.VMEM((2, 3, 4, 2, LANES, LANES), BF16),
                            pltpu.VMEM((layers, 2, 2 * LANES, 4 * LANES), BF16), pltpu.VMEM((layers, 2, 4 * LANES, 2 * LANES), BF16),
                            pltpu.VMEM((layers, 2, 8, LANES), F32),
                            pltpu.SMEM(gamma_angles.shape, F32), pltpu.SMEM(beta_angles.shape, F32),
                            pltpu.SemaphoreType.DMA, pltpu.SemaphoreType.DMA((2,)),
                            pltpu.SemaphoreType.DMA((half,)), pltpu.SemaphoreType.DMA((half,))],
            compiler_params=pltpu.CompilerParams(collective_id=0, has_side_effects=True, vmem_limit_bytes=32 * 1024 * 1024),
        )(*[pltpu.with_memory_space_constraint(x, pltpu.HBM) for x in (gamma_angles, beta_angles, cost_loc.reshape(rows, LANES))])
        energy, re, im = pl.pallas_call(
            write_kernel, out_shape=(jax.ShapeDtypeStruct((1,), F32), st, st),
            in_specs=[vmem, vmem, vmem], out_specs=(smem, vmem, vmem),
            compiler_params=pltpu.CompilerParams(vmem_limit_bytes=4 * 1024 * 1024),
        )(partial, re, im)
        return energy, re.reshape(local), im.reshape(local)

    return jax.shard_map(device_body, mesh=mesh, in_specs=(state_spec, P(), P()), out_specs=(P('inst'), state_spec, state_spec), check_vma=False)
```

```python
import functools
import math
import jax
import jax.numpy as jnp
from jax import lax
from jax.experimental import pallas as pl
from jax.experimental.pallas import tpu as pltpu
from jax.sharding import PartitionSpec as P

LANES = 128
QUAD = 4
SIN_POLY = (4.442883014678955, -7.308245658874512, 3.606354236602783, -0.8461116552352905, 0.1098245158791542)
COS_POLY = (1.4142135381698608, -6.9788641929626465, 5.73988151550293, -1.888274908065796, 0.33225154876708984, -0.034501612186431885)
F32 = jnp.float32
BF16 = jnp.bfloat16


def flip_bits(value, mask):
    bit = 1
    while bit <= mask:
        if mask & bit:
            value = value + bit * (1 - 2 * ((value // bit) % 2))
        bit *= 2
    return value


def turn_cos_sin(turns):
    rem = turns - jnp.round(turns)
    sq = rem * rem
    s = SIN_POLY[-1]
    for k in SIN_POLY[-2::-1]:
        s = s * sq + k
    s = s * rem
    c = COS_POLY[-1]
    for k in COS_POLY[-2::-1]:
        c = c * sq + k
    return 1.0 - s * s, s * c


def split3(x):
    a = x.astype(BF16)
    r = x - a.astype(F32)
    b = r.astype(BF16)
    c = (r - b.astype(F32)).astype(BF16)
    return a, b, c


def missing(diff, e):
    bits = [1 << b for b in range(e.bit_length()) if e >> b & 1]
    if len(bits) == 2:
        a, b = bits
        c = next(1 << k for k in range(4) if not e >> k & 1 and all(x in diff for x in (e | 1 << k, a | 1 << k, b | 1 << k)))
        return diff[e | c] - diff[a | c] - diff[b | c] + diff[a] + diff[b] + diff[c]
    pairs = [a | b for i, a in enumerate(bits) for b in bits[:i]]
    total = diff[pairs[0]]
    for p in pairs[1:]:
        total = total + diff[p]
    return total - (len(bits) - 2.0) * sum((diff[b] for b in bits[1:]), diff[bits[0]])


def reverse_rows(x):
    n = x.shape[0]
    i = lax.broadcasted_iota(jnp.int32, (n, n), 0)
    j = lax.broadcasted_iota(jnp.int32, (n, n), 1)
    perm = jnp.where(i + j == n - 1, 1.0, 0.0).astype(F32)
    return jnp.dot(perm, x, precision=lax.Precision.HIGHEST, preferred_element_type=F32)


def product_matrix(diag, off0, off1, scale):
    lane = lax.broadcasted_iota(jnp.int32, (8, LANES), 1)
    sub = lax.broadcasted_iota(jnp.int32, (8, LANES), 0)
    bit = lambda v, b: (v // (1 << b)) % 2
    base = jnp.full((8, LANES), 1.0, F32) * scale
    rows = [[None, None] for _ in range(7)]
    for b in range(7):
        lb = bit(lane, b) == 1
        row0 = jnp.where(lb, off0, diag[0])
        row1 = jnp.where(lb, diag[1], off1)
        rows[b] = [row0, row1]
    for b in range(3):
        base = base * jnp.where(bit(sub, b) == 1, rows[b][1], rows[b][0])
    blocks = [base]
    for b in range(3, 7):
        blocks = [x * rows[b][0] for x in blocks] + [x * rows[b][1] for x in blocks]
    return jnp.concatenate(blocks, axis=0)


CHUNKS = ((0, 64, ((0, 64),)), (64, 64, ((64, 32), (96, 32))))
LAST_CHUNKS = ((0, 64, ((0, 64),)), (64, 64, ((64, 48), (112, 16))))


def kernel(layers, total_bits, half, nqy, gamma_hbm, beta_hbm, cost_hbm, energy_ref, re_ref, im_ref,
           cost_ref, table_ref, diff_ref, packet, cst, base_ref, start_ref, low_ref, high_ref, ph_ref, sx, lx, w_ref, h_ref, trig_ref, gamma_ref, beta_ref,
           load_sem, angle_sem, send_sem, recv_sem):
    load = pltpu.make_async_copy(cost_hbm, cost_ref, load_sem)
    load.start()
    angle_loads = [pltpu.make_async_copy(gamma_hbm, gamma_ref, angle_sem.at[0]),
                   pltpu.make_async_copy(beta_hbm, beta_ref, angle_sem.at[1])]
    for angle_load in angle_loads:
        angle_load.start()
    me_x, me_y = lax.axis_index('qx'), lax.axis_index('qy')
    barrier = pltpu.get_barrier_semaphore()
    near = nqy // 2
    hops = {e: (0, 1, 2, 1)[e // (2 * near)] + e % near for e in range(1, half)}
    asked = [e for e in hops if hops[e] < 2 or (hops[e] == 2 and (e // near) % 2 == 0)]
    order = sorted(asked, key=lambda e: (-hops[e], e))
    partners = {e: {'qx': flip_bits(me_x, e // near), 'qy': flip_bits(me_y, e % near)} for e in order}
    for e in order:
        pl.semaphore_signal(barrier, inc=1, device_id=partners[e], device_id_type=pl.DeviceIdType.MESH)
    load.wait()
    rows = cost_ref.shape[0]
    row_bits = int(math.log2(rows))
    lane1 = lax.broadcasted_iota(jnp.int32, (1, LANES), 1)
    slopes = jnp.zeros((1, LANES), F32)
    for k in range(row_bits):
        row = cost_ref[(1 << k):(1 << k) + 1, :]
        slopes = jnp.where(lane1 == k, row if k == 0 else pltpu.roll(row, k, axis=1), slopes)
    packet[0:1, :] = cost_ref[0:1, :]
    packet[1:2, :] = slopes
    own = packet[...]
    pl.semaphore_wait(barrier, len(order))
    copies = {}
    for e in order:
        copies[e] = pltpu.make_async_remote_copy(
            src_ref=packet, dst_ref=table_ref.at[e], send_sem=send_sem.at[e], recv_sem=recv_sem.at[e],
            device_id=partners[e], device_id_type=pl.DeviceIdType.MESH)
        copies[e].start()
    for angle_load in angle_loads:
        angle_load.wait()
    zero = jnp.zeros((LANES, LANES), BF16)
    for l in range(layers):
        half_beta = jnp.full((8, LANES), 0.5, F32) * beta_ref[l]
        c, s = jnp.cos(half_beta), jnp.sin(half_beta)
        a = product_matrix((c, c), -s, s, c)
        b = product_matrix((-s, -s), -c, c, -s)
        a_t = product_matrix((c, c), s, -s, 0.25 * c)
        b_t = product_matrix((-s, -s), c, -c, -0.25 * s)
        for pq in range(2):
            g1, g2, g3 = split3(a - b if pq else a + b)
            w_ref[l, pq] = jnp.concatenate([jnp.concatenate([g1, g1, g1, zero], axis=1),
                                            jnp.concatenate([g2, g2, zero, g3], axis=1)], axis=0)
            h1, h2, h3 = split3(a_t - b_t if pq else a_t + b_t)
            h_ref[l, pq] = jnp.concatenate([jnp.concatenate([h1, h1, h1, zero], axis=0),
                                            jnp.concatenate([h2, h2, zero, h3], axis=0)], axis=1)
        trig_ref[l, 0] = c * c - s * s
        trig_ref[l, 1] = 2.0 * (s * c)

    lane = lax.broadcasted_iota(jnp.int32, (LANES, LANES), 1)
    vrow = lax.broadcasted_iota(jnp.int32, (LANES, LANES), 0)
    ones = jnp.zeros((LANES, LANES), jnp.int32)
    for b in range(7):
        ones = ones + (lane // (1 << b)) % 2 + (vrow // (1 << b)) % 2
    ones = ones % 4
    quarter = ones.astype(F32) * 0.25
    amp = 2.0 ** (-total_bits / 2.0)
    cost = cost_ref[...]
    bases = (cost, reverse_rows(cost))
    sub = lax.broadcasted_iota(jnp.int32, (8, LANES), 0)

    def unit(turns):
        co, si = turn_cos_sin(turns)
        return co, -si

    def mul(x, y):
        return x[0] * y[0] - x[1] * y[1], x[0] * y[1] + x[1] * y[0]

    rates = [gamma_ref[l] * (1.0 / (2.0 * math.pi)) for l in range(layers)]
    for t in range(2):
        for l in range(1, layers):
            for i, x in enumerate(unit(bases[t] * rates[l])):
                base_ref[l, t, i] = x
        turns = bases[t] * rates[0]
        turns = turns - jnp.round(turns) - quarter[:rows]
        re, im = unit(turns)
        re, im = amp * re, amp * im
        for e0s, pair in enumerate(((re, im), (-im, re))):
            for i, x in enumerate(pair):
                start_ref[t, e0s, i] = x

    def place(e):
        t = e // (2 * QUAD)
        return t, e % QUAD, (e // QUAD) % 2 ^ t

    def put_state(u, lo, x0, x1):
        n = x0.shape[0]
        for pq, x in enumerate((x0 + x1, x0 - x1)):
            for k, part in enumerate(split3(x)):
                sx[u, pq, k, lo:lo + n, :] = part

    def rows_stage(l, u):
        out = []
        for pq in range(2):
            x = [sx[u, pq, k] for k in range(3)]
            y = jnp.dot(w_ref[l, pq], jnp.concatenate(x + x[:1], axis=0), preferred_element_type=F32)
            out.append(y[:LANES] + y[LANES:])
        return out

    def put_pair(u, ys):
        (p0, q0), (p3, q3) = ys[u], ys[3 - u]
        for pq, v, y in ((0, u, p0 + p3), (0, 3 - u, q0 - q3), (1, u, q0 + q3), (1, 3 - u, p0 - p3)):
            for k, part in enumerate(split3(y)):
                for i in range(2):
                    lx[pq, k, v, i] = part[:, i * LANES:(i + 1) * LANES]

    def lanes_dot(l, pair, lo, n):
        out = {}
        for pq in range(2):
            x = [jnp.concatenate([lx[pq, k, u, i, lo:lo + n, :] for u in pair for i in range(2)], axis=0) for k in range(3)]
            z = jnp.dot(jnp.concatenate(x + x[:1], axis=1), h_ref[l, pq], preferred_element_type=F32)
            z = z[:, :LANES] + z[:, LANES:]
            for a, u in enumerate(pair):
                out[pq, u] = [z[(a * 2 + i) * n:(a * 2 + i + 1) * n] for i in range(2)]
        return out

    def mix_pairs(l, f):
        cb, sb = trig_ref[l, 0, 0:1, :], trig_ref[l, 1, 0:1, :]
        psi = []
        for pq in range(2):
            p, q, n, m = [f[pq, u] for u in range(4)]
            p, q = ((cb * p[0] + sb * q[1], cb * p[1] - sb * q[0]), (cb * q[0] + sb * p[1], cb * q[1] - sb * p[0]))
            psi.append([[p[i] + m[i] for i in range(2)], [q[i] + n[i] for i in range(2)],
                        [q[i] - n[i] for i in range(2)], [p[i] - m[i] for i in range(2)]])
        first = [[psi[0][u][i] + psi[1][u][i] for i in range(2)] for u in range(4)]
        second = [[psi[0][3 - u][i] - psi[1][3 - u][i] for i in range(2)] for u in range(4)]
        return first, second

    def lanes_stage(l):
        for start, size, chunks in CHUNKS if l < layers - 1 else LAST_CHUNKS:
            early = lanes_dot(l, (0, 3), start, size)
            for lo, n in chunks:
                f = lanes_dot(l, (1, 2), lo, n)
                for key, x in early.items():
                    f[key] = [y[lo - start:lo - start + n] for y in x]
                yield lo, n, mix_pairs(l, f)

    for e in order:
        copies[e].wait()
    diff = {0: jnp.zeros((2, LANES), F32)}
    for e in order:
        diff[e] = table_ref[e] - own
    for e in sorted(range(half), key=lambda e: bin(e).count('1')):
        if e not in diff:
            diff[e] = missing(diff, e)
        diff_ref[:, e] = diff[e]
    first = diff_ref[0]
    corner = jnp.broadcast_to(diff_ref[0, :, 0:1], (half, LANES))
    cols = [jnp.broadcast_to(diff_ref[1, :, k:k + 1], (half, LANES)) - corner for k in range(row_bits)]
    low = {}
    for e in range(1, half):
        part = jnp.broadcast_to(first[e:e + 1, :], (8, LANES))
        for k in range(3):
            part = part + jnp.where((sub // (1 << k)) % 2 == 1 - e // (2 * QUAD), cols[k][e:e + 1, :], 0.0)
        low[e] = part

    def put_factors(l):
        for k in range(3, row_bits):
            for i, x in enumerate(unit(cols[k] * rates[l])):
                high_ref[l, k - 3, i] = x
        for e in range(1, half):
            for i, x in enumerate(unit(low[e] * rates[l])):
                low_ref[l, e, i] = x

    def factors(l, e):
        out = [(low_ref[l, e, 0], low_ref[l, e, 1])]
        for k in range(row_bits - 3):
            h = (high_ref[l, k, 0, e:e + 1, :], high_ref[l, k, 1, e:e + 1, :])
            more = [mul(x, h) for x in out]
            out = more + out if e // (2 * QUAD) else out + more
        return [jnp.concatenate([x[i] for x in out], axis=0) for i in range(2)]

    def put_phases(l, us):
        for e in range(half):
            t, u, e0s = place(e)
            if u in us:
                x = (base_ref[l, t, 0], base_ref[l, t, 1])
                if e:
                    x = mul(x, factors(l, e))
                for i in range(2):
                    ph_ref[t, u, i, e0s * rows:(e0s + 1) * rows, :] = x[i]

    def put_cost(us):
        for e in range(half):
            t, u, e0s = place(e)
            if u in us:
                block = bases[t]
                if e:
                    parts = [low[e]]
                    for k in range(3, row_bits):
                        more = [x + cols[k][e:e + 1, :] for x in parts]
                        parts = more + parts if t else parts + more
                    block = block + jnp.concatenate(parts, axis=0)
                cst[t, u, e0s * rows:(e0s + 1) * rows, :] = block

    put_factors(0)
    ys = {}
    for u in (0, 3, 1, 2):
        xs = [[None, None], [None, None]]
        for e in range(half):
            if e % QUAD == u:
                t, _, e0s = place(e)
                x = (start_ref[t, e0s, 0], start_ref[t, e0s, 1])
                xs[t][e0s] = jnp.concatenate(mul(x, factors(0, e)) if e else x, axis=1)
        put_state(u, 0, *[jnp.concatenate(x, axis=0) for x in xs])
        ys[u] = rows_stage(0, u)
        if u == 3:
            put_pair(0, ys)
        if u == 2:
            put_pair(1, ys)
    put_factors(1)
    put_phases(1, range(QUAD))

    total = jnp.zeros((8, LANES), F32)
    for l in range(layers):
        for lo, n, both in lanes_stage(l):
            at = pl.ds(lo, n)
            if l < layers - 1:
                for u in range(4):
                    xs = []
                    for t in range(2):
                        a, b = both[t][u]
                        pr, pi = ph_ref[t, u, 0, at, :], ph_ref[t, u, 1, at, :]
                        xs.append(jnp.concatenate([a * pr - b * pi, b * pr + a * pi], axis=1))
                    put_state(u, lo, *xs)
            else:
                for u in range(4):
                    for t in range(2):
                        a, b = both[t][u]
                        total = total + jnp.sum((cst[t, u, at, :] * (a * a + b * b)).reshape(n // 8, 8, LANES), axis=0)
                if lo < rows:
                    a, b = both[0][0]
                    k = ones[lo:lo + n, :]
                    re_ref[at, :] = jnp.where(k == 0, a, jnp.where(k == 1, b, jnp.where(k == 2, -a, -b)))
                    im_ref[at, :] = jnp.where(k == 0, b, jnp.where(k == 1, -a, jnp.where(k == 2, -b, a)))
        if l < layers - 1:
            ys = {}
            for u in (0, 3, 1, 2):
                ys[u] = rows_stage(l + 1, u)
                if u == 3:
                    put_pair(0, ys)
                if u == 2:
                    put_pair(1, ys)
            if l + 2 < layers:
                put_factors(l + 2)
                put_phases(l + 2, range(QUAD))
            else:
                put_cost(range(QUAD))
    energy_ref[...] = total


def write_kernel(partial_ref, re_in, im_in, energy_ref, re_ref, im_ref):
    re_ref[...] = re_in[...]
    im_ref[...] = im_in[...]
    energy_ref[0] = 2.0 * jnp.sum(partial_ref[...])


def solution(mesh):
    nqx, nqy = mesh.shape['qx'], mesh.shape['qy']
    half = nqx * nqy // 2
    state_spec = P(('inst', 'qx', 'qy'))
    vmem = pl.BlockSpec(memory_space=pltpu.VMEM)
    smem = pl.BlockSpec(memory_space=pltpu.SMEM)
    hbm = pl.BlockSpec(memory_space=pltpu.HBM)

    def device_body(cost_loc, gamma_angles, beta_angles):
        local = cost_loc.shape[0]
        rows = local // LANES
        total_bits = int(math.log2(local * nqx * nqy))
        layers = gamma_angles.shape[0]
        st = jax.ShapeDtypeStruct((rows, LANES), F32)
        partial, re, im = pl.pallas_call(
            functools.partial(kernel, layers, total_bits, half, nqy),
            out_shape=(jax.ShapeDtypeStruct((8, LANES), F32), st, st),
            in_specs=[hbm, hbm, hbm], out_specs=(vmem, vmem, vmem),
            scratch_shapes=[pltpu.VMEM((rows, LANES), F32), pltpu.VMEM((half, 2, LANES), F32), pltpu.VMEM((2, half, LANES), F32), pltpu.VMEM((2, LANES), F32),
                            pltpu.VMEM((2, 4, LANES, LANES), F32),
                            pltpu.VMEM((layers, 2, 2, rows, LANES), F32), pltpu.VMEM((2, 2, 2, rows, LANES), F32),
                            pltpu.VMEM((layers, half, 2, 8, LANES), F32), pltpu.VMEM((layers, 3, 2, half, LANES), F32),
                            pltpu.VMEM((2, 4, 2, LANES, LANES), F32),
                            pltpu.VMEM((4, 2, 3, LANES, 2 * LANES), BF16), pltpu.VMEM((2, 3, 4, 2, LANES, LANES), BF16),
                            pltpu.VMEM((layers, 2, 2 * LANES, 4 * LANES), BF16), pltpu.VMEM((layers, 2, 4 * LANES, 2 * LANES), BF16),
                            pltpu.VMEM((layers, 2, 8, LANES), F32),
                            pltpu.SMEM(gamma_angles.shape, F32), pltpu.SMEM(beta_angles.shape, F32),
                            pltpu.SemaphoreType.DMA, pltpu.SemaphoreType.DMA((2,)),
                            pltpu.SemaphoreType.DMA((half,)), pltpu.SemaphoreType.DMA((half,))],
            compiler_params=pltpu.CompilerParams(collective_id=0, has_side_effects=True, vmem_limit_bytes=32 * 1024 * 1024),
        )(*[pltpu.with_memory_space_constraint(x, pltpu.HBM) for x in (gamma_angles, beta_angles, cost_loc.reshape(rows, LANES))])
        energy, re, im = pl.pallas_call(
            write_kernel, out_shape=(jax.ShapeDtypeStruct((1,), F32), st, st),
            in_specs=[vmem, vmem, vmem], out_specs=(smem, vmem, vmem),
            compiler_params=pltpu.CompilerParams(vmem_limit_bytes=4 * 1024 * 1024),
        )(partial, re, im)
        return energy, re.reshape(local), im.reshape(local)

    return jax.shard_map(device_body, mesh=mesh, in_specs=(state_spec, P(), P()), out_specs=(P('inst'), state_spec, state_spec), check_vma=False)
```

```python
import functools
import math
import jax
import jax.numpy as jnp
from jax import lax
from jax.experimental import pallas as pl
from jax.experimental.pallas import tpu as pltpu
from jax.sharding import PartitionSpec as P

LANES = 128
QUAD = 4
SIN_POLY = (4.442883014678955, -7.308245658874512, 3.606354236602783, -0.8461116552352905, 0.1098245158791542)
COS_POLY = (1.4142135381698608, -6.9788641929626465, 5.73988151550293, -1.888274908065796, 0.33225154876708984, -0.034501612186431885)
F32 = jnp.float32
BF16 = jnp.bfloat16


def flip_bits(value, mask):
    bit = 1
    while bit <= mask:
        if mask & bit:
            value = value + bit * (1 - 2 * ((value // bit) % 2))
        bit *= 2
    return value


def turn_cos_sin(turns):
    rem = turns - jnp.round(turns)
    sq = rem * rem
    s = SIN_POLY[-1]
    for k in SIN_POLY[-2::-1]:
        s = s * sq + k
    s = s * rem
    c = COS_POLY[-1]
    for k in COS_POLY[-2::-1]:
        c = c * sq + k
    return 1.0 - s * s, s * c


def split3(x):
    a = x.astype(BF16)
    r = x - a.astype(F32)
    b = r.astype(BF16)
    c = (r - b.astype(F32)).astype(BF16)
    return a, b, c


def missing(diff, e):
    bits = [1 << b for b in range(e.bit_length()) if e >> b & 1]
    if len(bits) == 2:
        a, b = bits
        c = next(1 << k for k in range(4) if not e >> k & 1 and all(x in diff for x in (e | 1 << k, a | 1 << k, b | 1 << k)))
        return diff[e | c] - diff[a | c] - diff[b | c] + diff[a] + diff[b] + diff[c]
    pairs = [a | b for i, a in enumerate(bits) for b in bits[:i]]
    total = diff[pairs[0]]
    for p in pairs[1:]:
        total = total + diff[p]
    return total - (len(bits) - 2.0) * sum((diff[b] for b in bits[1:]), diff[bits[0]])


def reverse_rows(x):
    n = x.shape[0]
    i = lax.broadcasted_iota(jnp.int32, (n, n), 0)
    j = lax.broadcasted_iota(jnp.int32, (n, n), 1)
    perm = jnp.where(i + j == n - 1, 1.0, 0.0).astype(F32)
    return jnp.dot(perm, x, precision=lax.Precision.HIGHEST, preferred_element_type=F32)


def product_matrix(diag, off0, off1, scale):
    lane = lax.broadcasted_iota(jnp.int32, (8, LANES), 1)
    sub = lax.broadcasted_iota(jnp.int32, (8, LANES), 0)
    bit = lambda v, b: (v // (1 << b)) % 2
    base = jnp.full((8, LANES), 1.0, F32) * scale
    rows = [[None, None] for _ in range(7)]
    for b in range(7):
        lb = bit(lane, b) == 1
        row0 = jnp.where(lb, off0, diag[0])
        row1 = jnp.where(lb, diag[1], off1)
        rows[b] = [row0, row1]
    for b in range(3):
        base = base * jnp.where(bit(sub, b) == 1, rows[b][1], rows[b][0])
    blocks = [base]
    for b in range(3, 7):
        blocks = [x * rows[b][0] for x in blocks] + [x * rows[b][1] for x in blocks]
    return jnp.concatenate(blocks, axis=0)


CHUNKS = ((0, 64, ((0, 64),)), (64, 32, ()), (96, 32, ()))
LAST_CHUNKS = ((0, 64, ((0, 64),)), (64, 64, ((64, 48), (112, 16))))


def kernel(layers, total_bits, half, nqy, gamma_hbm, beta_hbm, cost_hbm, energy_ref, re_ref, im_ref,
           cost_ref, table_ref, diff_ref, packet, cst, base_ref, start_ref, low_ref, high_ref, ph_ref, sx, lx, w_ref, h_ref, trig_ref, gamma_ref, beta_ref,
           load_sem, angle_sem, send_sem, recv_sem):
    load = pltpu.make_async_copy(cost_hbm, cost_ref, load_sem)
    load.start()
    angle_loads = [pltpu.make_async_copy(gamma_hbm, gamma_ref, angle_sem.at[0]),
                   pltpu.make_async_copy(beta_hbm, beta_ref, angle_sem.at[1])]
    for angle_load in angle_loads:
        angle_load.start()
    me_x, me_y = lax.axis_index('qx'), lax.axis_index('qy')
    barrier = pltpu.get_barrier_semaphore()
    near = nqy // 2
    hops = {e: (0, 1, 2, 1)[e // (2 * near)] + e % near for e in range(1, half)}
    asked = [e for e in hops if hops[e] < 2 or (hops[e] == 2 and (e // near) % 2 == 0)]
    order = sorted(asked, key=lambda e: (-hops[e], -e))
    partners = {e: {'qx': flip_bits(me_x, e // near), 'qy': flip_bits(me_y, e % near)} for e in order}
    for e in order:
        pl.semaphore_signal(barrier, inc=1, device_id=partners[e], device_id_type=pl.DeviceIdType.MESH)
    load.wait()
    rows = cost_ref.shape[0]
    row_bits = int(math.log2(rows))
    lane1 = lax.broadcasted_iota(jnp.int32, (1, LANES), 1)
    slopes = jnp.zeros((1, LANES), F32)
    for k in range(row_bits):
        row = cost_ref[(1 << k):(1 << k) + 1, :]
        slopes = jnp.where(lane1 == k, row if k == 0 else pltpu.roll(row, k, axis=1), slopes)
    packet[0:1, :] = cost_ref[0:1, :]
    packet[1:2, :] = slopes
    own = packet[...]
    pl.semaphore_wait(barrier, len(order))
    copies = {}
    for e in order:
        copies[e] = pltpu.make_async_remote_copy(
            src_ref=packet, dst_ref=table_ref.at[e], send_sem=send_sem.at[e], recv_sem=recv_sem.at[e],
            device_id=partners[e], device_id_type=pl.DeviceIdType.MESH)
        copies[e].start()
    for angle_load in angle_loads:
        angle_load.wait()
    zero = jnp.zeros((LANES, LANES), BF16)
    for l in range(layers):
        half_beta = jnp.full((8, LANES), 0.5, F32) * beta_ref[l]
        c, s = jnp.cos(half_beta), jnp.sin(half_beta)
        a = product_matrix((c, c), -s, s, c)
        b = product_matrix((-s, -s), -c, c, -s)
        a_t = product_matrix((c, c), s, -s, 0.25 * c)
        b_t = product_matrix((-s, -s), c, -c, -0.25 * s)
        for pq in range(2):
            g1, g2, g3 = split3(a - b if pq else a + b)
            w_ref[l, pq] = jnp.concatenate([jnp.concatenate([g1, g1, g1, zero], axis=1),
                                            jnp.concatenate([g2, g2, zero, g3], axis=1)], axis=0)
            h1, h2, h3 = split3(a_t - b_t if pq else a_t + b_t)
            h_ref[l, pq] = jnp.concatenate([jnp.concatenate([h1, h1, h1, zero], axis=0),
                                            jnp.concatenate([h2, h2, zero, h3], axis=0)], axis=1)
        trig_ref[l, 0] = c * c - s * s
        trig_ref[l, 1] = 2.0 * (s * c)

    lane = lax.broadcasted_iota(jnp.int32, (LANES, LANES), 1)
    vrow = lax.broadcasted_iota(jnp.int32, (LANES, LANES), 0)
    ones = jnp.zeros((LANES, LANES), jnp.int32)
    for b in range(7):
        ones = ones + (lane // (1 << b)) % 2 + (vrow // (1 << b)) % 2
    ones = ones % 4
    quarter = ones.astype(F32) * 0.25
    amp = 2.0 ** (-total_bits / 2.0)
    cost = cost_ref[...]
    bases = (cost, reverse_rows(cost))
    sub = lax.broadcasted_iota(jnp.int32, (8, LANES), 0)

    def unit(turns):
        co, si = turn_cos_sin(turns)
        return co, -si

    def mul(x, y):
        return x[0] * y[0] - x[1] * y[1], x[0] * y[1] + x[1] * y[0]

    rates = [gamma_ref[l] * (1.0 / (2.0 * math.pi)) for l in range(layers)]
    for t in range(2):
        for l in range(1, layers):
            for i, x in enumerate(unit(bases[t] * rates[l])):
                base_ref[l, t, i] = x
        turns = bases[t] * rates[0]
        turns = turns - jnp.round(turns) - quarter[:rows]
        re, im = unit(turns)
        re, im = amp * re, amp * im
        for e0s, pair in enumerate(((re, im), (-im, re))):
            for i, x in enumerate(pair):
                start_ref[t, e0s, i] = x

    def place(e):
        t = e // (2 * QUAD)
        return t, e % QUAD, (e // QUAD) % 2 ^ t

    def put_state(u, lo, x0, x1):
        n = x0.shape[0]
        for pq, x in enumerate((x0 + x1, x0 - x1)):
            for k, part in enumerate(split3(x)):
                sx[u, pq, k, lo:lo + n, :] = part

    def rows_stage(l, u):
        out = []
        for pq in range(2):
            x = [sx[u, pq, k] for k in range(3)]
            y = jnp.dot(w_ref[l, pq], jnp.concatenate(x + x[:1], axis=0), preferred_element_type=F32)
            out.append(y[:LANES] + y[LANES:])
        return out

    def put_pair(u, ys):
        (p0, q0), (p3, q3) = ys[u], ys[3 - u]
        for pq, v, y in ((0, u, p0 + p3), (0, 3 - u, q0 - q3), (1, u, q0 + q3), (1, 3 - u, p0 - p3)):
            for k, part in enumerate(split3(y)):
                for i in range(2):
                    lx[pq, k, v, i] = part[:, i * LANES:(i + 1) * LANES]

    def lanes_dot(l, pair, lo, n):
        out = {}
        for pq in range(2):
            x = [jnp.concatenate([lx[pq, k, u, i, lo:lo + n, :] for u in pair for i in range(2)], axis=0) for k in range(3)]
            z = jnp.dot(jnp.concatenate(x + x[:1], axis=1), h_ref[l, pq], preferred_element_type=F32)
            z = z[:, :LANES] + z[:, LANES:]
            for a, u in enumerate(pair):
                out[pq, u] = [z[(a * 2 + i) * n:(a * 2 + i + 1) * n] for i in range(2)]
        return out

    def mix_pairs(l, f):
        cb, sb = trig_ref[l, 0, 0:1, :], trig_ref[l, 1, 0:1, :]
        psi = []
        for pq in range(2):
            p, q, n, m = [f[pq, u] for u in range(4)]
            p, q = ((cb * p[0] + sb * q[1], cb * p[1] - sb * q[0]), (cb * q[0] + sb * p[1], cb * q[1] - sb * p[0]))
            psi.append([[p[i] + m[i] for i in range(2)], [q[i] + n[i] for i in range(2)],
                        [q[i] - n[i] for i in range(2)], [p[i] - m[i] for i in range(2)]])
        first = [[psi[0][u][i] + psi[1][u][i] for i in range(2)] for u in range(4)]
        second = [[psi[0][3 - u][i] - psi[1][3 - u][i] for i in range(2)] for u in range(4)]
        return first, second

    def lanes_stage(l):
        for start, size, chunks in CHUNKS if l < layers - 1 else LAST_CHUNKS:
            if not chunks:
                yield start, size, mix_pairs(l, lanes_dot(l, (0, 3, 1, 2), start, size))
                continue
            early = lanes_dot(l, (0, 3), start, size)
            for lo, n in chunks:
                f = lanes_dot(l, (1, 2), lo, n)
                for key, x in early.items():
                    f[key] = [y[lo - start:lo - start + n] for y in x]
                yield lo, n, mix_pairs(l, f)

    for e in order:
        copies[e].wait()
    diff = {0: jnp.zeros((2, LANES), F32)}
    for e in order:
        diff[e] = table_ref[e] - own
    for e in sorted(range(half), key=lambda e: bin(e).count('1')):
        if e not in diff:
            diff[e] = missing(diff, e)
        diff_ref[:, e] = diff[e]
    first = diff_ref[0]
    corner = jnp.broadcast_to(diff_ref[0, :, 0:1], (half, LANES))
    cols = [jnp.broadcast_to(diff_ref[1, :, k:k + 1], (half, LANES)) - corner for k in range(row_bits)]
    low = {}
    for e in range(1, half):
        part = jnp.broadcast_to(first[e:e + 1, :], (8, LANES))
        for k in range(3):
            part = part + jnp.where((sub // (1 << k)) % 2 == 1 - e // (2 * QUAD), cols[k][e:e + 1, :], 0.0)
        low[e] = part

    def put_factors(l):
        for k in range(3, row_bits):
            for i, x in enumerate(unit(cols[k] * rates[l])):
                high_ref[l, k - 3, i] = x
        for e in range(1, half):
            for i, x in enumerate(unit(low[e] * rates[l])):
                low_ref[l, e, i] = x

    def factors(l, e):
        out = [(low_ref[l, e, 0], low_ref[l, e, 1])]
        for k in range(row_bits - 3):
            h = (high_ref[l, k, 0, e:e + 1, :], high_ref[l, k, 1, e:e + 1, :])
            more = [mul(x, h) for x in out]
            out = more + out if e // (2 * QUAD) else out + more
        return [jnp.concatenate([x[i] for x in out], axis=0) for i in range(2)]

    def put_phases(l, us):
        for e in range(half):
            t, u, e0s = place(e)
            if u in us:
                x = (base_ref[l, t, 0], base_ref[l, t, 1])
                if e:
                    x = mul(x, factors(l, e))
                for i in range(2):
                    ph_ref[t, u, i, e0s * rows:(e0s + 1) * rows, :] = x[i]

    def put_cost(us):
        for e in range(half):
            t, u, e0s = place(e)
            if u in us:
                block = bases[t]
                if e:
                    parts = [low[e]]
                    for k in range(3, row_bits):
                        more = [x + cols[k][e:e + 1, :] for x in parts]
                        parts = more + parts if t else parts + more
                    block = block + jnp.concatenate(parts, axis=0)
                cst[t, u, e0s * rows:(e0s + 1) * rows, :] = block

    put_factors(0)
    ys = {}
    for u in (0, 3, 1, 2):
        xs = [[None, None], [None, None]]
        for e in range(half):
            if e % QUAD == u:
                t, _, e0s = place(e)
                x = (start_ref[t, e0s, 0], start_ref[t, e0s, 1])
                xs[t][e0s] = jnp.concatenate(mul(x, factors(0, e)) if e else x, axis=1)
        put_state(u, 0, *[jnp.concatenate(x, axis=0) for x in xs])
        ys[u] = rows_stage(0, u)
        if u == 3:
            put_pair(0, ys)
        if u == 2:
            put_pair(1, ys)
    put_factors(1)
    put_phases(1, range(QUAD))

    total = jnp.zeros((8, LANES), F32)
    for l in range(layers):
        for lo, n, both in lanes_stage(l):
            at = pl.ds(lo, n)
            if l < layers - 1:
                for u in range(4):
                    xs = []
                    for t in range(2):
                        a, b = both[t][u]
                        pr, pi = ph_ref[t, u, 0, at, :], ph_ref[t, u, 1, at, :]
                        xs.append(jnp.concatenate([a * pr - b * pi, b * pr + a * pi], axis=1))
                    put_state(u, lo, *xs)
            else:
                for u in range(4):
                    for t in range(2):
                        a, b = both[t][u]
                        total = total + jnp.sum((cst[t, u, at, :] * (a * a + b * b)).reshape(n // 8, 8, LANES), axis=0)
                if lo < rows:
                    a, b = both[0][0]
                    k = ones[lo:lo + n, :]
                    re_ref[at, :] = jnp.where(k == 0, a, jnp.where(k == 1, b, jnp.where(k == 2, -a, -b)))
                    im_ref[at, :] = jnp.where(k == 0, b, jnp.where(k == 1, -a, jnp.where(k == 2, -b, a)))
        if l < layers - 1:
            ys = {}
            for u in (0, 3, 1, 2):
                ys[u] = rows_stage(l + 1, u)
                if u == 3:
                    put_pair(0, ys)
                if u == 2:
                    put_pair(1, ys)
            if l + 2 < layers:
                put_factors(l + 2)
                put_phases(l + 2, range(QUAD))
            else:
                put_cost(range(QUAD))
    energy_ref[...] = total


def write_kernel(partial_ref, re_in, im_in, energy_ref, re_ref, im_ref):
    re_ref[...] = re_in[...]
    im_ref[...] = im_in[...]
    energy_ref[0] = 2.0 * jnp.sum(partial_ref[...])


def solution(mesh):
    nqx, nqy = mesh.shape['qx'], mesh.shape['qy']
    half = nqx * nqy // 2
    state_spec = P(('inst', 'qx', 'qy'))
    vmem = pl.BlockSpec(memory_space=pltpu.VMEM)
    smem = pl.BlockSpec(memory_space=pltpu.SMEM)
    hbm = pl.BlockSpec(memory_space=pltpu.HBM)

    def device_body(cost_loc, gamma_angles, beta_angles):
        local = cost_loc.shape[0]
        rows = local // LANES
        total_bits = int(math.log2(local * nqx * nqy))
        layers = gamma_angles.shape[0]
        st = jax.ShapeDtypeStruct((rows, LANES), F32)
        partial, re, im = pl.pallas_call(
            functools.partial(kernel, layers, total_bits, half, nqy),
            out_shape=(jax.ShapeDtypeStruct((8, LANES), F32), st, st),
            in_specs=[hbm, hbm, hbm], out_specs=(vmem, vmem, vmem),
            scratch_shapes=[pltpu.VMEM((rows, LANES), F32), pltpu.VMEM((half, 2, LANES), F32), pltpu.VMEM((2, half, LANES), F32), pltpu.VMEM((2, LANES), F32),
                            pltpu.VMEM((2, 4, LANES, LANES), F32),
                            pltpu.VMEM((layers, 2, 2, rows, LANES), F32), pltpu.VMEM((2, 2, 2, rows, LANES), F32),
                            pltpu.VMEM((layers, half, 2, 8, LANES), F32), pltpu.VMEM((layers, 3, 2, half, LANES), F32),
                            pltpu.VMEM((2, 4, 2, LANES, LANES), F32),
                            pltpu.VMEM((4, 2, 3, LANES, 2 * LANES), BF16), pltpu.VMEM((2, 3, 4, 2, LANES, LANES), BF16),
                            pltpu.VMEM((layers, 2, 2 * LANES, 4 * LANES), BF16), pltpu.VMEM((layers, 2, 4 * LANES, 2 * LANES), BF16),
                            pltpu.VMEM((layers, 2, 8, LANES), F32),
                            pltpu.SMEM(gamma_angles.shape, F32), pltpu.SMEM(beta_angles.shape, F32),
                            pltpu.SemaphoreType.DMA, pltpu.SemaphoreType.DMA((2,)),
                            pltpu.SemaphoreType.DMA((half,)), pltpu.SemaphoreType.DMA((half,))],
            compiler_params=pltpu.CompilerParams(collective_id=0, has_side_effects=True, vmem_limit_bytes=32 * 1024 * 1024),
        )(*[pltpu.with_memory_space_constraint(x, pltpu.HBM) for x in (gamma_angles, beta_angles, cost_loc.reshape(rows, LANES))])
        energy, re, im = pl.pallas_call(
            write_kernel, out_shape=(jax.ShapeDtypeStruct((1,), F32), st, st),
            in_specs=[vmem, vmem, vmem], out_specs=(smem, vmem, vmem),
            compiler_params=pltpu.CompilerParams(vmem_limit_bytes=4 * 1024 * 1024),
        )(partial, re, im)
        return energy, re.reshape(local), im.reshape(local)

    return jax.shard_map(device_body, mesh=mesh, in_specs=(state_spec, P(), P()), out_specs=(P('inst'), state_spec, state_spec), check_vma=False)
```

```python
import functools
import math
import jax
import jax.numpy as jnp
from jax import lax
from jax.experimental import pallas as pl
from jax.experimental.pallas import tpu as pltpu
from jax.sharding import PartitionSpec as P

LANES = 128
QUAD = 4
SIN_POLY = (4.442883014678955, -7.308245658874512, 3.606354236602783, -0.8461116552352905, 0.1098245158791542)
COS_POLY = (1.4142135381698608, -6.9788641929626465, 5.73988151550293, -1.888274908065796, 0.33225154876708984, -0.034501612186431885)
F32 = jnp.float32
BF16 = jnp.bfloat16


def flip_bits(value, mask):
    bit = 1
    while bit <= mask:
        if mask & bit:
            value = value + bit * (1 - 2 * ((value // bit) % 2))
        bit *= 2
    return value


def turn_cos_sin(turns):
    rem = turns - jnp.round(turns)
    sq = rem * rem
    s = SIN_POLY[-1]
    for k in SIN_POLY[-2::-1]:
        s = s * sq + k
    s = s * rem
    c = COS_POLY[-1]
    for k in COS_POLY[-2::-1]:
        c = c * sq + k
    return 1.0 - s * s, s * c


def split3(x):
    a = x.astype(BF16)
    r = x - a.astype(F32)
    b = r.astype(BF16)
    c = (r - b.astype(F32)).astype(BF16)
    return a, b, c


def missing(diff, e):
    bits = [1 << b for b in range(e.bit_length()) if e >> b & 1]
    if len(bits) == 2:
        a, b = bits
        c = next(1 << k for k in range(4) if not e >> k & 1 and all(x in diff for x in (e | 1 << k, a | 1 << k, b | 1 << k)))
        return diff[e | c] - diff[a | c] - diff[b | c] + diff[a] + diff[b] + diff[c]
    pairs = [a | b for i, a in enumerate(bits) for b in bits[:i]]
    total = diff[pairs[0]]
    for p in pairs[1:]:
        total = total + diff[p]
    return total - (len(bits) - 2.0) * sum((diff[b] for b in bits[1:]), diff[bits[0]])


def reverse_rows(x):
    n = x.shape[0]
    i = lax.broadcasted_iota(jnp.int32, (n, n), 0)
    j = lax.broadcasted_iota(jnp.int32, (n, n), 1)
    perm = jnp.where(i + j == n - 1, 1.0, 0.0).astype(F32)
    return jnp.dot(perm, x, precision=lax.Precision.HIGHEST, preferred_element_type=F32)


def product_matrix(diag, off0, off1, scale):
    lane = lax.broadcasted_iota(jnp.int32, (8, LANES), 1)
    sub = lax.broadcasted_iota(jnp.int32, (8, LANES), 0)
    bit = lambda v, b: (v // (1 << b)) % 2
    base = jnp.full((8, LANES), 1.0, F32) * scale
    rows = [[None, None] for _ in range(7)]
    for b in range(7):
        lb = bit(lane, b) == 1
        row0 = jnp.where(lb, off0, diag[0])
        row1 = jnp.where(lb, diag[1], off1)
        rows[b] = [row0, row1]
    for b in range(3):
        base = base * jnp.where(bit(sub, b) == 1, rows[b][1], rows[b][0])
    blocks = [base]
    for b in range(3, 7):
        blocks = [x * rows[b][0] for x in blocks] + [x * rows[b][1] for x in blocks]
    return jnp.concatenate(blocks, axis=0)


CHUNKS = ((0, 64, ((0, 64),)), (64, 32, ()), (96, 32, ()))
LAST_CHUNKS = ((0, 64, ((0, 64),)), (64, 64, ((64, 48), (112, 16))))


def kernel(layers, total_bits, half, nqy, gamma_hbm, beta_hbm, cost_hbm, energy_ref, re_ref, im_ref,
           cost_ref, table_ref, diff_ref, packet, cst, base_ref, start_ref, low_ref, high_ref, ph_ref, sx, lx, w_ref, h_ref, trig_ref, gamma_ref, beta_ref,
           load_sem, angle_sem, send_sem, recv_sem):
    load = pltpu.make_async_copy(cost_hbm, cost_ref, load_sem)
    load.start()
    angle_loads = [pltpu.make_async_copy(gamma_hbm, gamma_ref, angle_sem.at[0]),
                   pltpu.make_async_copy(beta_hbm, beta_ref, angle_sem.at[1])]
    for angle_load in angle_loads:
        angle_load.start()
    me_x, me_y = lax.axis_index('qx'), lax.axis_index('qy')
    barrier = pltpu.get_barrier_semaphore()
    near = nqy // 2
    hops = {e: (0, 1, 2, 1)[e // (2 * near)] + e % near for e in range(1, half)}
    asked = [e for e in hops if hops[e] < 2 or (hops[e] == 2 and (e // near) % 2 == 0)]
    order = sorted(asked, key=lambda e: (-hops[e], -e))
    partners = {e: {'qx': flip_bits(me_x, e // near), 'qy': flip_bits(me_y, e % near)} for e in order}
    for e in order:
        pl.semaphore_signal(barrier, inc=1, device_id=partners[e], device_id_type=pl.DeviceIdType.MESH)
    load.wait()
    rows = cost_ref.shape[0]
    row_bits = int(math.log2(rows))
    lane1 = lax.broadcasted_iota(jnp.int32, (1, LANES), 1)
    slopes = jnp.zeros((1, LANES), F32)
    for k in range(row_bits):
        row = cost_ref[(1 << k):(1 << k) + 1, :]
        slopes = jnp.where(lane1 == k, row if k == 0 else pltpu.roll(row, k, axis=1), slopes)
    packet[0:1, :] = cost_ref[0:1, :]
    packet[1:2, :] = slopes
    own = packet[...]
    pl.semaphore_wait(barrier, len(order))
    copies = {}
    for e in order:
        copies[e] = pltpu.make_async_remote_copy(
            src_ref=packet, dst_ref=table_ref.at[e], send_sem=send_sem.at[e], recv_sem=recv_sem.at[e],
            device_id=partners[e], device_id_type=pl.DeviceIdType.MESH)
        copies[e].start()
    for angle_load in angle_loads:
        angle_load.wait()
    zero = jnp.zeros((LANES, LANES), BF16)
    for l in range(layers):
        half_beta = jnp.full((8, LANES), 0.5, F32) * beta_ref[l]
        c, s = jnp.cos(half_beta), jnp.sin(half_beta)
        a = product_matrix((c, c), -s, s, c)
        b = product_matrix((-s, -s), -c, c, -s)
        a_t = product_matrix((c, c), s, -s, 0.25 * c)
        b_t = product_matrix((-s, -s), c, -c, -0.25 * s)
        for pq in range(2):
            g1, g2, g3 = split3(a - b if pq else a + b)
            w_ref[l, pq] = jnp.concatenate([jnp.concatenate([g1, g1, g1, zero], axis=1),
                                            jnp.concatenate([g2, g2, zero, g3], axis=1)], axis=0)
            h1, h2, h3 = split3(a_t - b_t if pq else a_t + b_t)
            h_ref[l, pq] = jnp.concatenate([jnp.concatenate([h1, h1, h1, zero], axis=0),
                                            jnp.concatenate([h2, h2, zero, h3], axis=0)], axis=1)
        trig_ref[l, 0] = c * c - s * s
        trig_ref[l, 1] = 2.0 * (s * c)

    lane = lax.broadcasted_iota(jnp.int32, (LANES, LANES), 1)
    vrow = lax.broadcasted_iota(jnp.int32, (LANES, LANES), 0)
    ones = jnp.zeros((LANES, LANES), jnp.int32)
    for b in range(7):
        ones = ones + (lane // (1 << b)) % 2 + (vrow // (1 << b)) % 2
    ones = ones % 4
    quarter = ones.astype(F32) * 0.25
    amp = 2.0 ** (-total_bits / 2.0)
    cost = cost_ref[...]
    bases = (cost, reverse_rows(cost))
    sub = lax.broadcasted_iota(jnp.int32, (8, LANES), 0)

    def mul(x, y):
        return x[0] * y[0] - x[1] * y[1], x[0] * y[1] + x[1] * y[0]

    rates = [gamma_ref[l] * (-1.0 / (2.0 * math.pi)) for l in range(layers)]
    for t in range(2):
        for l in range(1, layers):
            for i, x in enumerate(turn_cos_sin(bases[t] * rates[l])):
                base_ref[l, t, i] = x
        turns = bases[t] * rates[0]
        turns = turns - jnp.round(turns) + quarter[:rows]
        re, im = turn_cos_sin(turns)
        re, im = amp * re, amp * im
        for e0s, pair in enumerate(((re, im), (-im, re))):
            for i, x in enumerate(pair):
                start_ref[t, e0s, i] = x

    def place(e):
        t = e // (2 * QUAD)
        return t, e % QUAD, (e // QUAD) % 2 ^ t

    def put_state(u, lo, x0, x1):
        n = x0.shape[0]
        for pq, x in enumerate((x0 + x1, x0 - x1)):
            for k, part in enumerate(split3(x)):
                sx[u, pq, k, lo:lo + n, :] = part

    def rows_stage(l, u):
        out = []
        for pq in range(2):
            x = [sx[u, pq, k] for k in range(3)]
            y = jnp.dot(w_ref[l, pq], jnp.concatenate(x + x[:1], axis=0), preferred_element_type=F32)
            out.append(y[:LANES] + y[LANES:])
        return out

    def put_pair(u, ys):
        (p0, q0), (p3, q3) = ys[u], ys[3 - u]
        for pq, v, y in ((0, u, p0 + p3), (0, 3 - u, q0 - q3), (1, u, q0 + q3), (1, 3 - u, p0 - p3)):
            for k, part in enumerate(split3(y)):
                for i in range(2):
                    lx[pq, k, v, i] = part[:, i * LANES:(i + 1) * LANES]

    def lanes_dot(l, pair, lo, n):
        out = {}
        for pq in range(2):
            x = [jnp.concatenate([lx[pq, k, u, i, lo:lo + n, :] for u in pair for i in range(2)], axis=0) for k in range(3)]
            z = jnp.dot(jnp.concatenate(x + x[:1], axis=1), h_ref[l, pq], preferred_element_type=F32)
            z = z[:, :LANES] + z[:, LANES:]
            for a, u in enumerate(pair):
                out[pq, u] = [z[(a * 2 + i) * n:(a * 2 + i + 1) * n] for i in range(2)]
        return out

    def mix_pairs(l, f):
        cb, sb = trig_ref[l, 0, 0:1, :], trig_ref[l, 1, 0:1, :]
        psi = []
        for pq in range(2):
            p, q, n, m = [f[pq, u] for u in range(4)]
            p, q = ((cb * p[0] + sb * q[1], cb * p[1] - sb * q[0]), (cb * q[0] + sb * p[1], cb * q[1] - sb * p[0]))
            psi.append([[p[i] + m[i] for i in range(2)], [q[i] + n[i] for i in range(2)],
                        [q[i] - n[i] for i in range(2)], [p[i] - m[i] for i in range(2)]])
        first = [[psi[0][u][i] + psi[1][u][i] for i in range(2)] for u in range(4)]
        second = [[psi[0][3 - u][i] - psi[1][3 - u][i] for i in range(2)] for u in range(4)]
        return first, second

    def lanes_stage(l):
        for start, size, chunks in CHUNKS if l < layers - 1 else LAST_CHUNKS:
            if not chunks:
                yield start, size, mix_pairs(l, lanes_dot(l, (0, 3, 1, 2), start, size))
                continue
            early = lanes_dot(l, (0, 3), start, size)
            for lo, n in chunks:
                f = lanes_dot(l, (1, 2), lo, n)
                for key, x in early.items():
                    f[key] = [y[lo - start:lo - start + n] for y in x]
                yield lo, n, mix_pairs(l, f)

    for e in order:
        copies[e].wait_recv()
    diff = {0: jnp.zeros((2, LANES), F32)}
    for e in order:
        diff[e] = table_ref[e] - own
    for e in sorted(range(half), key=lambda e: bin(e).count('1')):
        if e not in diff:
            diff[e] = missing(diff, e)
        diff_ref[:, e] = diff[e]
    first = diff_ref[0]
    corner = jnp.broadcast_to(diff_ref[0, :, 0:1], (half, LANES))
    cols = [jnp.broadcast_to(diff_ref[1, :, k:k + 1], (half, LANES)) - corner for k in range(row_bits)]
    low = {}
    for e in range(1, half):
        part = jnp.broadcast_to(first[e:e + 1, :], (8, LANES))
        for k in range(3):
            part = part + jnp.where((sub // (1 << k)) % 2 == 1 - e // (2 * QUAD), cols[k][e:e + 1, :], 0.0)
        low[e] = part

    def put_factors(l):
        for k in range(3, row_bits):
            for i, x in enumerate(turn_cos_sin(cols[k] * rates[l])):
                high_ref[l, k - 3, i] = x
        for e in range(1, half):
            for i, x in enumerate(turn_cos_sin(low[e] * rates[l])):
                low_ref[l, e, i] = x

    def factors(l, e):
        out = [(low_ref[l, e, 0], low_ref[l, e, 1])]
        for k in range(row_bits - 3):
            h = (high_ref[l, k, 0, e:e + 1, :], high_ref[l, k, 1, e:e + 1, :])
            more = [mul(x, h) for x in out]
            out = more + out if e // (2 * QUAD) else out + more
        return [jnp.concatenate([x[i] for x in out], axis=0) for i in range(2)]

    def put_phases(l, us):
        for e in range(half):
            t, u, e0s = place(e)
            if u in us:
                x = (base_ref[l, t, 0], base_ref[l, t, 1])
                if e:
                    x = mul(x, factors(l, e))
                for i in range(2):
                    ph_ref[t, u, i, e0s * rows:(e0s + 1) * rows, :] = x[i]

    def put_cost(us):
        for e in range(half):
            t, u, e0s = place(e)
            if u in us:
                block = bases[t]
                if e:
                    parts = [low[e]]
                    for k in range(3, row_bits):
                        more = [x + cols[k][e:e + 1, :] for x in parts]
                        parts = more + parts if t else parts + more
                    block = block + jnp.concatenate(parts, axis=0)
                cst[t, u, e0s * rows:(e0s + 1) * rows, :] = block

    put_factors(0)
    ys = {}
    for u in (0, 3, 1, 2):
        xs = [[None, None], [None, None]]
        for e in range(half):
            if e % QUAD == u:
                t, _, e0s = place(e)
                x = (start_ref[t, e0s, 0], start_ref[t, e0s, 1])
                xs[t][e0s] = jnp.concatenate(mul(x, factors(0, e)) if e else x, axis=1)
        put_state(u, 0, *[jnp.concatenate(x, axis=0) for x in xs])
        ys[u] = rows_stage(0, u)
        if u == 3:
            put_pair(0, ys)
        if u == 2:
            put_pair(1, ys)
    put_factors(1)
    put_phases(1, range(QUAD))

    total = jnp.zeros((8, LANES), F32)
    for l in range(layers):
        for lo, n, both in lanes_stage(l):
            at = pl.ds(lo, n)
            if l < layers - 1:
                for u in range(4):
                    xs = []
                    for t in range(2):
                        a, b = both[t][u]
                        pr, pi = ph_ref[t, u, 0, at, :], ph_ref[t, u, 1, at, :]
                        xs.append(jnp.concatenate([a * pr - b * pi, b * pr + a * pi], axis=1))
                    put_state(u, lo, *xs)
            else:
                for u in range(4):
                    for t in range(2):
                        a, b = both[t][u]
                        total = total + jnp.sum((cst[t, u, at, :] * (a * a + b * b)).reshape(n // 8, 8, LANES), axis=0)
                if lo < rows:
                    a, b = both[0][0]
                    k = ones[lo:lo + n, :]
                    re_ref[at, :] = jnp.where(k == 0, a, jnp.where(k == 1, b, jnp.where(k == 2, -a, -b)))
                    im_ref[at, :] = jnp.where(k == 0, b, jnp.where(k == 1, -a, jnp.where(k == 2, -b, a)))
        if l < layers - 1:
            ys = {}
            for u in (0, 3, 1, 2):
                ys[u] = rows_stage(l + 1, u)
                if u == 3:
                    put_pair(0, ys)
                if u == 2:
                    put_pair(1, ys)
            if l + 2 < layers:
                put_factors(l + 2)
                put_phases(l + 2, range(QUAD))
            else:
                put_cost(range(QUAD))
    energy_ref[...] = total
    for e in order:
        copies[e].wait_send()


def write_kernel(partial_ref, re_in, im_in, energy_ref, re_ref, im_ref):
    re_ref[...] = re_in[...]
    im_ref[...] = im_in[...]
    energy_ref[0] = 2.0 * jnp.sum(partial_ref[...])


def solution(mesh):
    nqx, nqy = mesh.shape['qx'], mesh.shape['qy']
    half = nqx * nqy // 2
    state_spec = P(('inst', 'qx', 'qy'))
    vmem = pl.BlockSpec(memory_space=pltpu.VMEM)
    smem = pl.BlockSpec(memory_space=pltpu.SMEM)
    hbm = pl.BlockSpec(memory_space=pltpu.HBM)

    def device_body(cost_loc, gamma_angles, beta_angles):
        local = cost_loc.shape[0]
        rows = local // LANES
        total_bits = int(math.log2(local * nqx * nqy))
        layers = gamma_angles.shape[0]
        st = jax.ShapeDtypeStruct((rows, LANES), F32)
        partial, re, im = pl.pallas_call(
            functools.partial(kernel, layers, total_bits, half, nqy),
            out_shape=(jax.ShapeDtypeStruct((8, LANES), F32), st, st),
            in_specs=[hbm, hbm, hbm], out_specs=(vmem, vmem, vmem),
            scratch_shapes=[pltpu.VMEM((rows, LANES), F32), pltpu.VMEM((half, 2, LANES), F32), pltpu.VMEM((2, half, LANES), F32), pltpu.VMEM((2, LANES), F32),
                            pltpu.VMEM((2, 4, LANES, LANES), F32),
                            pltpu.VMEM((layers, 2, 2, rows, LANES), F32), pltpu.VMEM((2, 2, 2, rows, LANES), F32),
                            pltpu.VMEM((layers, half, 2, 8, LANES), F32), pltpu.VMEM((layers, 3, 2, half, LANES), F32),
                            pltpu.VMEM((2, 4, 2, LANES, LANES), F32),
                            pltpu.VMEM((4, 2, 3, LANES, 2 * LANES), BF16), pltpu.VMEM((2, 3, 4, 2, LANES, LANES), BF16),
                            pltpu.VMEM((layers, 2, 2 * LANES, 4 * LANES), BF16), pltpu.VMEM((layers, 2, 4 * LANES, 2 * LANES), BF16),
                            pltpu.VMEM((layers, 2, 8, LANES), F32),
                            pltpu.SMEM(gamma_angles.shape, F32), pltpu.SMEM(beta_angles.shape, F32),
                            pltpu.SemaphoreType.DMA, pltpu.SemaphoreType.DMA((2,)),
                            pltpu.SemaphoreType.DMA((half,)), pltpu.SemaphoreType.DMA((half,))],
            compiler_params=pltpu.CompilerParams(collective_id=0, has_side_effects=True, vmem_limit_bytes=32 * 1024 * 1024),
        )(*[pltpu.with_memory_space_constraint(x, pltpu.HBM) for x in (gamma_angles, beta_angles, cost_loc.reshape(rows, LANES))])
        energy, re, im = pl.pallas_call(
            write_kernel, out_shape=(jax.ShapeDtypeStruct((1,), F32), st, st),
            in_specs=[vmem, vmem, vmem], out_specs=(smem, vmem, vmem),
            compiler_params=pltpu.CompilerParams(vmem_limit_bytes=4 * 1024 * 1024),
        )(partial, re, im)
        return energy, re.reshape(local), im.reshape(local)

    return jax.shard_map(device_body, mesh=mesh, in_specs=(state_spec, P(), P()), out_specs=(P('inst'), state_spec, state_spec), check_vma=False)
```

```python
import functools
import math
import jax
import jax.numpy as jnp
from jax import lax
from jax.experimental import pallas as pl
from jax.experimental.pallas import tpu as pltpu
from jax.sharding import PartitionSpec as P

LANES = 128
QUAD = 4
SIN_POLY = (4.442883014678955, -7.308245658874512, 3.606354236602783, -0.8461116552352905, 0.1098245158791542)
COS_POLY = (1.4142135381698608, -6.9788641929626465, 5.73988151550293, -1.888274908065796, 0.33225154876708984, -0.034501612186431885)
F32 = jnp.float32
BF16 = jnp.bfloat16


def flip_bits(value, mask):
    bit = 1
    while bit <= mask:
        if mask & bit:
            value = value + bit * (1 - 2 * ((value // bit) % 2))
        bit *= 2
    return value


def turn_cos_sin(turns):
    rem = turns - jnp.round(turns)
    sq = rem * rem
    s = SIN_POLY[-1]
    for k in SIN_POLY[-2::-1]:
        s = s * sq + k
    s = s * rem
    c = COS_POLY[-1]
    for k in COS_POLY[-2::-1]:
        c = c * sq + k
    return 1.0 - s * s, s * c


def split3(x):
    a = x.astype(BF16)
    r = x - a.astype(F32)
    b = r.astype(BF16)
    c = (r - b.astype(F32)).astype(BF16)
    return a, b, c


def missing(diff, e):
    bits = [1 << b for b in range(e.bit_length()) if e >> b & 1]
    if len(bits) == 2:
        a, b = bits
        c = next(1 << k for k in range(4) if not e >> k & 1 and all(x in diff for x in (e | 1 << k, a | 1 << k, b | 1 << k)))
        return diff[e | c] - diff[a | c] - diff[b | c] + diff[a] + diff[b] + diff[c]
    pairs = [a | b for i, a in enumerate(bits) for b in bits[:i]]
    total = diff[pairs[0]]
    for p in pairs[1:]:
        total = total + diff[p]
    return total - (len(bits) - 2.0) * sum((diff[b] for b in bits[1:]), diff[bits[0]])


def reverse_rows(x):
    n = x.shape[0]
    i = lax.broadcasted_iota(jnp.int32, (n, n), 0)
    j = lax.broadcasted_iota(jnp.int32, (n, n), 1)
    perm = jnp.where(i + j == n - 1, 1.0, 0.0).astype(F32)
    return jnp.dot(perm, x, precision=lax.Precision.HIGHEST, preferred_element_type=F32)


def product_matrix(diag, off0, off1, scale):
    lane = lax.broadcasted_iota(jnp.int32, (8, LANES), 1)
    sub = lax.broadcasted_iota(jnp.int32, (8, LANES), 0)
    bit = lambda v, b: (v // (1 << b)) % 2
    base = jnp.full((8, LANES), 1.0, F32) * scale
    rows = [[None, None] for _ in range(7)]
    for b in range(7):
        lb = bit(lane, b) == 1
        row0 = jnp.where(lb, off0, diag[0])
        row1 = jnp.where(lb, diag[1], off1)
        rows[b] = [row0, row1]
    for b in range(3):
        base = base * jnp.where(bit(sub, b) == 1, rows[b][1], rows[b][0])
    blocks = [base]
    for b in range(3, 7):
        blocks = [x * rows[b][0] for x in blocks] + [x * rows[b][1] for x in blocks]
    return jnp.concatenate(blocks, axis=0)


CHUNKS = ((0, 64, ((0, 64),)), (64, 32, ()), (96, 32, ()))
LAST_CHUNKS = ((0, 64, ((0, 64),)), (64, 48, ()), (112, 16, ()))


def kernel(layers, total_bits, half, nqy, gamma_hbm, beta_hbm, cost_hbm, energy_ref, re_ref, im_ref,
           cost_ref, table_ref, diff_ref, packet, cst, base_ref, start_ref, low_ref, high_ref, ph_ref, sx, lx, w_ref, h_ref, trig_ref, gamma_ref, beta_ref,
           load_sem, angle_sem, send_sem, recv_sem):
    load = pltpu.make_async_copy(cost_hbm, cost_ref, load_sem)
    load.start()
    angle_loads = [pltpu.make_async_copy(gamma_hbm, gamma_ref, angle_sem.at[0]),
                   pltpu.make_async_copy(beta_hbm, beta_ref, angle_sem.at[1])]
    for angle_load in angle_loads:
        angle_load.start()
    me_x, me_y = lax.axis_index('qx'), lax.axis_index('qy')
    barrier = pltpu.get_barrier_semaphore()
    near = nqy // 2
    hops = {e: (0, 1, 2, 1)[e // (2 * near)] + e % near for e in range(1, half)}
    asked = [e for e in hops if hops[e] < 2 or (hops[e] == 2 and (e // near) % 2 == 0)]
    order = sorted(asked, key=lambda e: (-hops[e], -e))
    partners = {e: {'qx': flip_bits(me_x, e // near), 'qy': flip_bits(me_y, e % near)} for e in order}
    for e in order:
        pl.semaphore_signal(barrier, inc=1, device_id=partners[e], device_id_type=pl.DeviceIdType.MESH)
    load.wait()
    rows = cost_ref.shape[0]
    row_bits = int(math.log2(rows))
    lane1 = lax.broadcasted_iota(jnp.int32, (1, LANES), 1)
    slopes = jnp.zeros((1, LANES), F32)
    for k in range(row_bits):
        row = cost_ref[(1 << k):(1 << k) + 1, :]
        slopes = jnp.where(lane1 == k, row if k == 0 else pltpu.roll(row, k, axis=1), slopes)
    packet[0:1, :] = cost_ref[0:1, :]
    packet[1:2, :] = slopes
    own = packet[...]
    pl.semaphore_wait(barrier, len(order))
    copies = {}
    for e in order:
        copies[e] = pltpu.make_async_remote_copy(
            src_ref=packet, dst_ref=table_ref.at[e], send_sem=send_sem.at[e], recv_sem=recv_sem.at[e],
            device_id=partners[e], device_id_type=pl.DeviceIdType.MESH)
        copies[e].start()
    for angle_load in angle_loads:
        angle_load.wait()
    zero = jnp.zeros((LANES, LANES), BF16)
    for l in range(layers):
        half_beta = jnp.full((8, LANES), 0.5, F32) * beta_ref[l]
        c, s = jnp.cos(half_beta), jnp.sin(half_beta)
        a = product_matrix((c, c), -s, s, c)
        b = product_matrix((-s, -s), -c, c, -s)
        a_t = product_matrix((c, c), s, -s, 0.25 * c)
        b_t = product_matrix((-s, -s), c, -c, -0.25 * s)
        for pq in range(2):
            g1, g2, g3 = split3(a - b if pq else a + b)
            w_ref[l, pq] = jnp.concatenate([jnp.concatenate([g1, g1, g1, zero], axis=1),
                                            jnp.concatenate([g2, g2, zero, g3], axis=1)], axis=0)
            h1, h2, h3 = split3(a_t - b_t if pq else a_t + b_t)
            h_ref[l, pq] = jnp.concatenate([jnp.concatenate([h1, h1, h1, zero], axis=0),
                                            jnp.concatenate([h2, h2, zero, h3], axis=0)], axis=1)
        trig_ref[l, 0] = c * c - s * s
        trig_ref[l, 1] = 2.0 * (s * c)

    lane = lax.broadcasted_iota(jnp.int32, (LANES, LANES), 1)
    vrow = lax.broadcasted_iota(jnp.int32, (LANES, LANES), 0)
    ones = jnp.zeros((LANES, LANES), jnp.int32)
    for b in range(7):
        ones = ones + (lane // (1 << b)) % 2 + (vrow // (1 << b)) % 2
    ones = ones % 4
    quarter = ones.astype(F32) * 0.25
    amp = 2.0 ** (-total_bits / 2.0)
    cost = cost_ref[...]
    bases = (cost, reverse_rows(cost))
    sub = lax.broadcasted_iota(jnp.int32, (8, LANES), 0)

    def unit(turns):
        co, si = turn_cos_sin(turns)
        return co, -si

    def mul(x, y):
        return x[0] * y[0] - x[1] * y[1], x[0] * y[1] + x[1] * y[0]

    rates = [gamma_ref[l] * (1.0 / (2.0 * math.pi)) for l in range(layers)]
    for t in range(2):
        for l in range(1, layers):
            for i, x in enumerate(unit(bases[t] * rates[l])):
                base_ref[l, t, i] = x
        turns = bases[t] * rates[0]
        turns = turns - jnp.round(turns) - quarter[:rows]
        re, im = unit(turns)
        re, im = amp * re, amp * im
        for e0s, pair in enumerate(((re, im), (-im, re))):
            for i, x in enumerate(pair):
                start_ref[t, e0s, i] = x

    def place(e):
        t = e // 2 % 2
        return t, e // 4, e % 2 ^ t

    def put_state(u, lo, x0, x1):
        n = x0.shape[0]
        for pq, x in enumerate((x0 + x1, x0 - x1)):
            for k, part in enumerate(split3(x)):
                sx[u, pq, k, lo:lo + n, :] = part

    def rows_stage(l, u):
        out = []
        for pq in range(2):
            x = [sx[u, pq, k] for k in range(3)]
            y = jnp.dot(w_ref[l, pq], jnp.concatenate(x + x[:1], axis=0), preferred_element_type=F32)
            out.append(y[:LANES] + y[LANES:])
        return out

    def put_pair(u, ys):
        (p0, q0), (p3, q3) = ys[u], ys[3 - u]
        for pq, v, y in ((0, u, p0 + p3), (0, 3 - u, q0 - q3), (1, u, q0 + q3), (1, 3 - u, p0 - p3)):
            for k, part in enumerate(split3(y)):
                for i in range(2):
                    lx[pq, k, v, i] = part[:, i * LANES:(i + 1) * LANES]

    def lanes_dot(l, pair, lo, n):
        out = {}
        for pq in range(2):
            x = [jnp.concatenate([lx[pq, k, u, i, lo:lo + n, :] for u in pair for i in range(2)], axis=0) for k in range(3)]
            z = jnp.dot(jnp.concatenate(x + x[:1], axis=1), h_ref[l, pq], preferred_element_type=F32)
            z = z[:, :LANES] + z[:, LANES:]
            for a, u in enumerate(pair):
                out[pq, u] = [z[(a * 2 + i) * n:(a * 2 + i + 1) * n] for i in range(2)]
        return out

    def mix_pairs(l, f):
        cb, sb = trig_ref[l, 0, 0:1, :], trig_ref[l, 1, 0:1, :]
        psi = []
        for pq in range(2):
            p, q, n, m = [f[pq, u] for u in range(4)]
            p, q = ((cb * p[0] + sb * q[1], cb * p[1] - sb * q[0]), (cb * q[0] + sb * p[1], cb * q[1] - sb * p[0]))
            psi.append([[p[i] + m[i] for i in range(2)], [q[i] + n[i] for i in range(2)],
                        [q[i] - n[i] for i in range(2)], [p[i] - m[i] for i in range(2)]])
        first = [[psi[0][u][i] + psi[1][u][i] for i in range(2)] for u in range(4)]
        second = [[psi[0][3 - u][i] - psi[1][3 - u][i] for i in range(2)] for u in range(4)]
        return first, second

    def lanes_stage(l):
        for start, size, chunks in CHUNKS if l < layers - 1 else LAST_CHUNKS:
            if not chunks:
                yield start, size, mix_pairs(l, lanes_dot(l, (0, 3, 1, 2), start, size))
                continue
            early = lanes_dot(l, (0, 3), start, size)
            for lo, n in chunks:
                f = lanes_dot(l, (1, 2), lo, n)
                for key, x in early.items():
                    f[key] = [y[lo - start:lo - start + n] for y in x]
                yield lo, n, mix_pairs(l, f)

    for e in order:
        copies[e].wait()
    diff = {0: jnp.zeros((2, LANES), F32)}
    for e in order:
        diff[e] = table_ref[e] - own
    for e in sorted(range(half), key=lambda e: bin(e).count('1')):
        if e not in diff:
            diff[e] = missing(diff, e)
        diff_ref[:, e] = diff[e]
    first = diff_ref[0]
    corner = jnp.broadcast_to(diff_ref[0, :, 0:1], (half, LANES))
    cols = [jnp.broadcast_to(diff_ref[1, :, k:k + 1], (half, LANES)) - corner for k in range(row_bits)]
    low = {}
    for e in range(1, half):
        part = jnp.broadcast_to(first[e:e + 1, :], (8, LANES))
        for k in range(3):
            part = part + jnp.where((sub // (1 << k)) % 2 == 1 - place(e)[0], cols[k][e:e + 1, :], 0.0)
        low[e] = part

    def put_factors(l):
        for k in range(3, row_bits):
            for i, x in enumerate(unit(cols[k] * rates[l])):
                high_ref[l, k - 3, i] = x
        for e in range(1, half):
            for i, x in enumerate(unit(low[e] * rates[l])):
                low_ref[l, e, i] = x

    def factors(l, e):
        out = [(low_ref[l, e, 0], low_ref[l, e, 1])]
        for k in range(row_bits - 3):
            h = (high_ref[l, k, 0, e:e + 1, :], high_ref[l, k, 1, e:e + 1, :])
            more = [mul(x, h) for x in out]
            out = more + out if place(e)[0] else out + more
        return [jnp.concatenate([x[i] for x in out], axis=0) for i in range(2)]

    def put_phases(l, us):
        for e in range(half):
            t, u, e0s = place(e)
            if u in us:
                x = (base_ref[l, t, 0], base_ref[l, t, 1])
                if e:
                    x = mul(x, factors(l, e))
                for i in range(2):
                    ph_ref[t, u, i, e0s * rows:(e0s + 1) * rows, :] = x[i]

    def put_cost(us):
        for e in range(half):
            t, u, e0s = place(e)
            if u in us:
                block = bases[t]
                if e:
                    parts = [low[e]]
                    for k in range(3, row_bits):
                        more = [x + cols[k][e:e + 1, :] for x in parts]
                        parts = more + parts if t else parts + more
                    block = block + jnp.concatenate(parts, axis=0)
                cst[t, u, e0s * rows:(e0s + 1) * rows, :] = block

    put_factors(0)
    ys = {}
    for u in (0, 3, 1, 2):
        xs = [[None, None], [None, None]]
        for e in range(half):
            if place(e)[1] == u:
                t, _, e0s = place(e)
                x = (start_ref[t, e0s, 0], start_ref[t, e0s, 1])
                xs[t][e0s] = jnp.concatenate(mul(x, factors(0, e)) if e else x, axis=1)
        put_state(u, 0, *[jnp.concatenate(x, axis=0) for x in xs])
        ys[u] = rows_stage(0, u)
        if u == 3:
            put_pair(0, ys)
        if u == 2:
            put_pair(1, ys)
    put_factors(1)
    put_phases(1, range(QUAD))

    total = jnp.zeros((8, LANES), F32)
    for l in range(layers):
        for lo, n, both in lanes_stage(l):
            at = pl.ds(lo, n)
            if l < layers - 1:
                for u in range(4):
                    xs = []
                    for t in range(2):
                        a, b = both[t][u]
                        pr, pi = ph_ref[t, u, 0, at, :], ph_ref[t, u, 1, at, :]
                        xs.append(jnp.concatenate([a * pr - b * pi, b * pr + a * pi], axis=1))
                    put_state(u, lo, *xs)
            else:
                for u in range(4):
                    for t in range(2):
                        a, b = both[t][u]
                        total = total + jnp.sum((cst[t, u, at, :] * (a * a + b * b)).reshape(n // 8, 8, LANES), axis=0)
                if lo < rows:
                    a, b = both[0][0]
                    k = ones[lo:lo + n, :]
                    re_ref[at, :] = jnp.where(k == 0, a, jnp.where(k == 1, b, jnp.where(k == 2, -a, -b)))
                    im_ref[at, :] = jnp.where(k == 0, b, jnp.where(k == 1, -a, jnp.where(k == 2, -b, a)))
        if l < layers - 1:
            ys = {}
            for u in (0, 3, 1, 2):
                ys[u] = rows_stage(l + 1, u)
                if u == 3:
                    put_pair(0, ys)
                if u == 2:
                    put_pair(1, ys)
            if l + 2 < layers:
                put_factors(l + 2)
                put_phases(l + 2, range(QUAD))
            else:
                put_cost(range(QUAD))
    energy_ref[...] = total


def write_kernel(partial_ref, re_in, im_in, energy_ref, re_ref, im_ref):
    re_ref[...] = re_in[...]
    im_ref[...] = im_in[...]
    energy_ref[0] = 2.0 * jnp.sum(partial_ref[...])


def solution(mesh):
    nqx, nqy = mesh.shape['qx'], mesh.shape['qy']
    half = nqx * nqy // 2
    state_spec = P(('inst', 'qx', 'qy'))
    vmem = pl.BlockSpec(memory_space=pltpu.VMEM)
    smem = pl.BlockSpec(memory_space=pltpu.SMEM)
    hbm = pl.BlockSpec(memory_space=pltpu.HBM)

    def device_body(cost_loc, gamma_angles, beta_angles):
        local = cost_loc.shape[0]
        rows = local // LANES
        total_bits = int(math.log2(local * nqx * nqy))
        layers = gamma_angles.shape[0]
        st = jax.ShapeDtypeStruct((rows, LANES), F32)
        partial, re, im = pl.pallas_call(
            functools.partial(kernel, layers, total_bits, half, nqy),
            out_shape=(jax.ShapeDtypeStruct((8, LANES), F32), st, st),
            in_specs=[hbm, hbm, hbm], out_specs=(vmem, vmem, vmem),
            scratch_shapes=[pltpu.VMEM((rows, LANES), F32), pltpu.VMEM((half, 2, LANES), F32), pltpu.VMEM((2, half, LANES), F32), pltpu.VMEM((2, LANES), F32),
                            pltpu.VMEM((2, 4, LANES, LANES), F32),
                            pltpu.VMEM((layers, 2, 2, rows, LANES), F32), pltpu.VMEM((2, 2, 2, rows, LANES), F32),
                            pltpu.VMEM((layers, half, 2, 8, LANES), F32), pltpu.VMEM((layers, 3, 2, half, LANES), F32),
                            pltpu.VMEM((2, 4, 2, LANES, LANES), F32),
                            pltpu.VMEM((4, 2, 3, LANES, 2 * LANES), BF16), pltpu.VMEM((2, 3, 4, 2, LANES, LANES), BF16),
                            pltpu.VMEM((layers, 2, 2 * LANES, 4 * LANES), BF16), pltpu.VMEM((layers, 2, 4 * LANES, 2 * LANES), BF16),
                            pltpu.VMEM((layers, 2, 8, LANES), F32),
                            pltpu.SMEM(gamma_angles.shape, F32), pltpu.SMEM(beta_angles.shape, F32),
                            pltpu.SemaphoreType.DMA, pltpu.SemaphoreType.DMA((2,)),
                            pltpu.SemaphoreType.DMA((half,)), pltpu.SemaphoreType.DMA((half,))],
            compiler_params=pltpu.CompilerParams(collective_id=0, has_side_effects=True, vmem_limit_bytes=32 * 1024 * 1024),
        )(*[pltpu.with_memory_space_constraint(x, pltpu.HBM) for x in (gamma_angles, beta_angles, cost_loc.reshape(rows, LANES))])
        energy, re, im = pl.pallas_call(
            write_kernel, out_shape=(jax.ShapeDtypeStruct((1,), F32), st, st),
            in_specs=[vmem, vmem, vmem], out_specs=(smem, vmem, vmem),
            compiler_params=pltpu.CompilerParams(vmem_limit_bytes=4 * 1024 * 1024),
        )(partial, re, im)
        return energy, re.reshape(local), im.reshape(local)

    return jax.shard_map(device_body, mesh=mesh, in_specs=(state_spec, P(), P()), out_specs=(P('inst'), state_spec, state_spec), check_vma=False)
```
